32 devices in a mesh: batch: 4 (over y, z), seq: 8 (over x, core).
Axes of the slice: x: 4, y: 2, z: 2, core: 2. Of those that a mesh axis runs over, the one named last changes fastest.
The devices are a block of a 4x4x8 slice.
Arguments:
- hidden: bfloat16 [64, 5120], P('batch'), parts along dimension 0
- lengths: int32 [64], P('batch'), parts along dimension 0
- c_kv: bfloat16 [64, 8192, 512], P('batch', 'seq'), parts along dimension 0
- k_rope: bfloat16 [64, 8192, 64], P('batch', 'seq'), parts along dimension 0
- w_uq: bfloat16 [5120, 128, 128], P(None, 'seq')
- w_qr: bfloat16 [5120, 128, 64], P(None, 'seq')
- w_uk: bfloat16 [128, 128, 512], P('seq')
- w_uv: bfloat16 [128, 512, 128], P('seq')
- w_o: bfloat16 [128, 128, 5120], P('seq')
Outputs:
- output: bfloat16 [64, 5120], P('batch'), parts along dimension 0
There are 4 independent parts. The reference program is written for one: setup_inputs(seed, part) draws one part's arguments, and reference() takes and returns one part's arrays. A program takes and returns all parts, laid end to end along the dimension named above; an argument that names none is the same for every part.
All inputs are finite; a program needn't handle non-finite values.
Results may differ from the reference program's by a relative error of at most 0.00434223.
Values are sent between devices in bfloat16 or wider.
A program may use at most 768 MiB of HBM per device.

```python
import math
import jax
import jax.numpy as jnp
from jax import lax

BATCH_ROWS = 16
D_MODEL = 5120
NUM_HEADS = 128
SHARD_LEN = 1024
CACHE_LEN = 8192
LATENT_DIM = 512
ROPE_DIM = 64
NOPE_DIM = 128
VALUE_DIM = 128
SCORE_SCALE = 1.0 / math.sqrt(NOPE_DIM + ROPE_DIM)
SCORE_GAIN = 0.75 * math.sqrt(math.log(CACHE_LEN))


def draw_lengths(len_key):
    perm_key, long_key, short_key = jax.random.split(len_key, 3)
    row_rank = jax.random.permutation(perm_key, BATCH_ROWS)
    long_len = jax.random.randint(long_key, (BATCH_ROWS,), CACHE_LEN - SHARD_LEN + 1, CACHE_LEN + 1)
    long_len = jnp.where(row_rank == 0, CACHE_LEN, long_len)
    short_len = jax.random.randint(short_key, (BATCH_ROWS,), 1, CACHE_LEN // 4 + 1)
    return jnp.where(row_rank < max(1, BATCH_ROWS // 4), long_len, short_len).astype(jnp.int32)


def setup_inputs(seed: int = 0, part: int = 0) -> dict:
    part_key = jax.random.fold_in(jax.random.key(seed), part)
    key_list = jax.random.split(part_key, 4)
    weight_keys = jax.random.split(jax.random.key(seed + 1), 5)
    hidden = jax.random.normal(key_list[0], (BATCH_ROWS, D_MODEL), jnp.float32)
    c_kv = jax.random.normal(key_list[2], (BATCH_ROWS, CACHE_LEN, LATENT_DIM), jnp.float32)
    k_rope = jax.random.normal(key_list[3], (BATCH_ROWS, CACHE_LEN, ROPE_DIM), jnp.float32)
    w_uq = jax.random.normal(weight_keys[0], (D_MODEL, NUM_HEADS, NOPE_DIM), jnp.float32) * D_MODEL ** -0.5
    w_qr = jax.random.normal(weight_keys[1], (D_MODEL, NUM_HEADS, ROPE_DIM), jnp.float32) * D_MODEL ** -0.5
    w_uk = jax.random.normal(weight_keys[2], (NUM_HEADS, NOPE_DIM, LATENT_DIM), jnp.float32) * (SCORE_GAIN * NOPE_DIM ** -0.5)
    w_uv = jax.random.normal(weight_keys[3], (NUM_HEADS, LATENT_DIM, VALUE_DIM), jnp.float32) * LATENT_DIM ** -0.5
    w_o = jax.random.normal(weight_keys[4], (NUM_HEADS, VALUE_DIM, D_MODEL), jnp.float32) * (NUM_HEADS * VALUE_DIM) ** -0.5
    return dict(hidden=hidden.astype(jnp.bfloat16), lengths=draw_lengths(key_list[1]), c_kv=c_kv.astype(jnp.bfloat16), k_rope=k_rope.astype(jnp.bfloat16), w_uq=w_uq.astype(jnp.bfloat16), w_qr=w_qr.astype(jnp.bfloat16), w_uk=w_uk.astype(jnp.bfloat16), w_uv=w_uv.astype(jnp.bfloat16), w_o=w_o.astype(jnp.bfloat16))


def reference(hidden, lengths, c_kv, k_rope, w_uq, w_qr, w_uk, w_uv, w_o):
    hidden_f32 = hidden.astype(jnp.float32)
    q_nope = jnp.einsum('bd,dhk->bhk', hidden_f32, w_uq.astype(jnp.float32)).astype(jnp.bfloat16)
    q_rope = jnp.einsum('bd,dhr->bhr', hidden_f32, w_qr.astype(jnp.float32)).astype(jnp.bfloat16)
    q_lat = jnp.einsum('bhk,hkc->bhc', q_nope.astype(jnp.float32), w_uk.astype(jnp.float32)).astype(jnp.bfloat16)
    positions = jnp.arange(CACHE_LEN)

    def one_row(row_args):
        q_lat_row, q_rope_row, c_row, k_row, row_len = row_args
        scores = (jnp.dot(q_lat_row, c_row.T, preferred_element_type=jnp.float32) + jnp.dot(q_rope_row, k_row.T, preferred_element_type=jnp.float32)) * SCORE_SCALE
        scores = jnp.where(positions[None, :] < row_len, scores, -jnp.inf)
        row_max = jnp.max(scores, axis=1, keepdims=True)
        p_weights = jnp.exp(scores - row_max)
        weight_sum = jnp.sum(p_weights, axis=1, keepdims=True)
        latent_sum = jnp.dot(p_weights.astype(jnp.bfloat16), c_row, preferred_element_type=jnp.float32)
        return (latent_sum / weight_sum).astype(jnp.bfloat16)

    o_lat = lax.map(one_row, (q_lat, q_rope, c_kv, k_rope, lengths))
    o_val = jnp.einsum('bhc,hcv->bhv', o_lat.astype(jnp.float32), w_uv.astype(jnp.float32)).astype(jnp.bfloat16)
    y_sum = jnp.einsum('bhv,hvd->bd', o_val.astype(jnp.float32), w_o.astype(jnp.float32))
    return (hidden_f32 + y_sum).astype(jnp.bfloat16)
```

```python
import functools
import math

import jax
import jax.numpy as jnp
from jax import lax
from jax.experimental import pallas as pl
from jax.experimental.pallas import tpu as pltpu
from jax.sharding import PartitionSpec as P

MESH = pl.DeviceIdType.MESH
F32 = jnp.float32
BF16 = jnp.bfloat16
LOWEST = float(jnp.finfo(jnp.float32).min)
DCH = 256
SLOTS = 8
RPC = 2


def iota(shape, dim):
    return lax.broadcasted_iota(jnp.int32, shape, dim)


def dot(a, b):
    return lax.dot_general(a, b, (((1,), (0,)), ((), ())), preferred_element_type=F32)


def dot_nt(a, b):
    return lax.dot_general(a, b, (((1,), (1,)), ((), ())), preferred_element_type=F32)


def merge(blocks, lat):
    rows = []
    for r in range(RPC):
        base = RPC * lat
        ms = [b[:, base + r:base + r + 1] for b in blocks]
        ls = [b[:, base + RPC + r:base + RPC + r + 1] for b in blocks]
        m = functools.reduce(jnp.maximum, ms)
        ws = [jnp.exp(x - m) for x in ms]
        l = functools.reduce(lambda a, b: a + b, [w * y for w, y in zip(ws, ls)])
        o = functools.reduce(lambda a, b: a + b,
                             [w * b[:, r * lat:(r + 1) * lat] for w, b in zip(ws, blocks)])
        rows.append((o, m, l))
    return rows


def pack_ml(ms, ls, shape):
    lane = iota(shape, 1)
    out = jnp.zeros(shape, F32)
    for r in range(RPC):
        out = jnp.where(lane == r, ms[r], out)
        out = jnp.where(lane == RPC + r, ls[r], out)
    return out


def kernel(n, scale, lens, hid, c_hbm, k_hbm, wuq_hbm, wqr_hbm, wuk_hbm, wuv_hbm, wo_hbm, out_ref,
           hexp, wbuf, wuk, wuv, wo, cb, kb, acc, q_all, qr_st, qr_all, qrow, o_buf, d2d, mid, fin, ol, ovb,
           y_send, y_recv, y_own, out_all,
           w_sem, wuk_sem, wqr_sem, c_sem, k_sem, wuv_sem, wo_sem,
           ag_s, ag_r, rs_s, d2d_r, mid_r, fin_r, y_s, y_r, g_s, g_r):
    s = lax.axis_index("seq")
    x, c = lax.div(s, 2), lax.rem(s, 2)
    nx = n // 2
    oc = 1 - c
    xr, xl, xo = lax.rem(x + 1, nx), lax.rem(x + nx - 1, nx), lax.rem(x + 2, nx)
    partner, right, left = 2 * x + oc, 2 * xr + c, 2 * xl + c
    rows, dm = hid.shape
    t_len, lat = cb.shape[1], cb.shape[2]
    nheads = 16 * n
    nc = dm // DCH
    nch = rows // RPC

    def remote(src, dst, ssem, rsem, dev):
        return pltpu.make_async_remote_copy(src_ref=src, dst_ref=dst, send_sem=ssem, recv_sem=rsem,
                                            device_id={"seq": dev}, device_id_type=MESH)

    def w_copy(g):
        half, i = lax.div(g, nc), lax.rem(g, nc)
        return pltpu.make_async_copy(wuq_hbm.at[pl.ds(i * DCH, DCH), half], wbuf.at[lax.rem(g, SLOTS)],
                                     w_sem.at[lax.rem(g, SLOTS)])

    def wuk_copy(half):
        return pltpu.make_async_copy(wuk_hbm.at[half], wuk.at[half], wuk_sem.at[half])

    def wqr_copy(j):
        return pltpu.make_async_copy(wqr_hbm.at[pl.ds(j * 128, 128)], wo.at[pl.ds(j * 128, 128)], wqr_sem.at[j])

    def c_copy(b):
        return pltpu.make_async_copy(c_hbm.at[b], cb.at[b], c_sem.at[b])

    def k_copy(b):
        return pltpu.make_async_copy(k_hbm.at[b], kb.at[b], k_sem.at[b])

    def wo_copy(j):
        return pltpu.make_async_copy(wo_hbm.at[pl.ds(j * 256, 256)], wo.at[pl.ds(j * 256, 256)], wo_sem.at[j])

    wuk_copy(0).start()
    for g in range(SLOTS):
        w_copy(jnp.int32(g)).start()

    barrier = pltpu.get_barrier_semaphore()
    for d in range(1, n):
        pl.semaphore_signal(barrier, inc=1, device_id={"seq": lax.rem(s + d, n)}, device_id_type=MESH)

    rep = jnp.where(iota((128, 1024), 0) == lax.div(iota((128, 1024), 1), 8), 1.0, 0.0).astype(BF16)
    ndt = dm // 128
    for g0 in range(0, ndt, 8):
        grp = list(range(g0, min(g0 + 8, ndt)))
        st = jnp.concatenate([hid[:, t * 128:(t + 1) * 128] for t in grp], axis=0)
        ex = dot(st, rep).astype(BF16)
        for i, t in enumerate(grp):
            hexp[:, t * 1024:(t + 1) * 1024] = ex[i * 16:(i + 1) * 16]

    head_mask = jnp.where(lax.div(iota((128, 128), 0), 16) == lax.rem(iota((128, 128), 1), 8), 1.0, 0.0).astype(BF16)
    ri, ci = iota((128, 128), 0), iota((128, 128), 1)
    to_bh = jnp.where(ci == lax.rem(ri, 8) * 16 + lax.div(ri, 8), 1.0, 0.0).astype(BF16)
    to_hb = jnp.where(ci == lax.rem(ri, 16) * 8 + lax.div(ri, 16), 1.0, 0.0).astype(BF16)
    row_h = lax.rem(iota((128, 1), 0), 8)

    pl.semaphore_wait(barrier, n - 1)

    def ag_buf(t, owner):
        return qr_all.at[owner] if t == 2 else q_all.at[owner, t]

    def ag(t, i, owner, dev):
        return remote(ag_buf(t, owner), ag_buf(t, owner), ag_s.at[t, i], ag_r.at[t, owner], dev)

    def ag_own(t):
        ag(t, 0, s, right).start()
        ag(t, 1, s, left).start()
        ag(t, 2, s, partner).start()

    def ag_fwd1(t):
        ag(t, 0, left, right).wait_recv()
        ag(t, 3, left, partner).start()
        if t != 1:
            ag(t, 5, left, right).start()
        ag(t, 1, right, left).wait_recv()
        ag(t, 4, right, partner).start()
        if t == 1:
            ag(t, 5, right, left).start()

    opp = 2 * xo + c

    def ag_fwd2(t):
        ag(t, 5, opp, right).wait_recv()
        ag(t, 6, opp, partner).start()

    def ag_partner(t):
        for xx in (x, xl, xr, xo):
            ag(t, 2, 2 * xx + oc, partner).wait_recv()

    def ag_done(t):
        for i in range(7):
            ag(t, i, s, partner).wait_send()

    kk = DCH * 8
    def half_step(half):
        acc[...] = jnp.zeros_like(acc)

        @pl.loop(0, nc)
        def _(i):
            g = half * nc + i
            slot = lax.rem(g, SLOTS)
            w_copy(g).wait()
            wv = wbuf[slot].reshape(kk, 128)
            part = acc[...]
            for q0 in range(0, kk, 512):
                hx = hexp[:, pl.ds(pl.multiple_of(i * kk + q0, 512), 512)]
                lhs = jnp.concatenate([hx] * 8, axis=0) * jnp.concatenate([head_mask] * 4, axis=1)
                part += dot(lhs, wv[q0:q0 + 512])
            acc[...] = part

            @pl.when(g + SLOTS < 2 * nc)
            def _():
                w_copy(g + SLOTS).start()

            @pl.when(g >= 2 * nc - 8)
            def _():
                wqr_copy(g - (2 * nc - 8)).start()

            if half == 0:
                @pl.when(i == 4)
                def _():
                    wuk_copy(1).start()
            else:
                @pl.when(i == nc // 2 + 2)
                def _():
                    ag_fwd1(0)

                @pl.when(i == nc - 1)
                def _():
                    ag_fwd2(0)

        qn = dot(to_bh, acc[...].astype(BF16)).astype(BF16)
        wuk_copy(half).wait()
        ql = jnp.zeros((128, lat), F32)
        for h in range(8):
            ql += dot(jnp.where(row_h == h, qn, jnp.zeros_like(qn)), wuk[half, h * 128:(h + 1) * 128, :])
        q_all[s, half] = ql.astype(BF16)
        ag_own(half)

    half_step(0)
    half_step(1)

    @pl.loop(0, 8)
    def _(j):
        wqr_copy(j).wait()
        qr = dot_nt(hid[...], wo[pl.ds(pl.multiple_of(j * 128, 128), 128), :])
        qr_st[pl.ds(pl.multiple_of(j * 16, 16), 16), :] = qr.astype(BF16)
        for r in range(2):
            b = 2 * j + r
            c_copy(b).start()
            k_copy(b).start()

        @pl.when(j == 5)
        def _():
            ag_fwd1(1)

    qr_all[s] = dot(to_bh, qr_st[...]).astype(BF16)
    ag_own(2)
    pltpu.make_async_copy(wuv_hbm, wuv, wuv_sem).start()
    ag_fwd2(1)
    ag_fwd1(2)
    ag_fwd2(2)
    for t in range(3):
        ag_partner(t)

    dup = jnp.where(lax.div(iota((128, 64), 0), 2) == iota((128, 64), 1), 1.0, 0.0).astype(BF16)
    rope_mask = jnp.where(lax.rem(iota((128, 128), 0), 2) == lax.div(iota((128, 128), 1), 64), 1.0, 0.0)
    pos = s * t_len + iota((1, t_len), 1)
    width = RPC * lat + 128

    def attend(k):
        k16 = pl.ds(pl.multiple_of(k * 16, 16), 16)
        for p in range(n):
            qa = q_all[p, 0, k16, :].astype(F32)
            qb = q_all[p, 1, k16, :].astype(F32)
            for r in range(RPC):
                qrow[r, p * 16:(p + 1) * 16, :] = jnp.concatenate(
                    [qa[r * 8:(r + 1) * 8], qb[r * 8:(r + 1) * 8]], axis=0).astype(BF16)
        mls = []
        for r in range(RPC):
            b = k * RPC + r
            c_copy(b).wait()
            k_copy(b).wait()
            pairs = jnp.concatenate(
                [qr_all[p, k16, :].astype(F32)[r * 8:(r + 1) * 8] for p in range(n)], axis=0).astype(BF16)
            qr = (dot(dup, pairs) * rope_mask).astype(BF16)
            keys = kb[b]
            sc = dot_nt(qrow[r], cb[b]) + dot(qr, jnp.concatenate([keys, keys], axis=0))
            sc = jnp.where(pos < lens[b], sc * scale, -jnp.inf)
            m = jnp.maximum(jnp.max(sc, axis=1, keepdims=True), LOWEST)
            pw = jnp.exp(sc - m)
            l = jnp.sum(pw, axis=1, keepdims=True)
            o = dot(pw.astype(BF16), cb[b])
            for p in range(n):
                for ab in range(2):
                    h0 = p * 16 + ab * 8
                    o_buf[k, p % 2, p // 2, ab, :, r * lat:(r + 1) * lat] = o[h0:h0 + 8]
            mls.append((m, l))
        ml = pack_ml([a for a, _ in mls], [a for _, a in mls], (nheads, 128))
        for p in range(n):
            for ab in range(2):
                h0 = p * 16 + ab * 8
                o_buf[k, p % 2, p // 2, ab, :, RPC * lat:] = ml[h0:h0 + 8]

    def d2d_copy(k):
        return remote(o_buf.at[k, oc], d2d.at[k], rs_s.at[k, 0], d2d_r.at[k], partner)

    def hop_copies(k):
        return [
            remote(o_buf.at[k, c, xo, 1], mid.at[k, 0], rs_s.at[k, 1], mid_r.at[k, 0], right),
            remote(o_buf.at[k, c, xo, 0], mid.at[k, 1], rs_s.at[k, 2], mid_r.at[k, 1], left),
            remote(o_buf.at[k, c, xr, 0], fin.at[k, 0], rs_s.at[k, 3], fin_r.at[k, 0], right),
            remote(o_buf.at[k, c, xl, 1], fin.at[k, 1], rs_s.at[k, 4], fin_r.at[k, 1], left),
        ]

    def mid_copies(k):
        return [
            remote(o_buf.at[k, c, xr, 1], fin.at[k, 2], rs_s.at[k, 5], fin_r.at[k, 2], right),
            remote(o_buf.at[k, c, xl, 0], fin.at[k, 3], rs_s.at[k, 6], fin_r.at[k, 3], left),
        ]

    def store_merged(k, xx, ab, other):
        ref = o_buf.at[k, c, xx, ab]
        res = merge([ref[...], other], lat)
        for r in range(RPC):
            ref[:, r * lat:(r + 1) * lat] = res[r][0]
        ref[:, RPC * lat:] = pack_ml([a[1] for a in res], [a[2] for a in res], (8, 128))

    def pair_stage(k):
        d2d_copy(k).wait_recv()
        for xx in range(nx):
            for ab in range(2):
                store_merged(k, xx, ab, d2d[k, xx, ab])
        for cp in hop_copies(k):
            cp.start()

    def mid_stage(k):
        hops, mids = hop_copies(k), mid_copies(k)
        hops[0].wait_recv()
        store_merged(k, xr, 1, mid[k, 0])
        mids[0].start()
        hops[1].wait_recv()
        store_merged(k, xl, 0, mid[k, 1])
        mids[1].start()

    def final_stage(k):
        hops, mids = hop_copies(k), mid_copies(k)
        hops[2].wait_recv()
        hops[3].wait_recv()
        mids[0].wait_recv()
        mids[1].wait_recv()
        for ab, (f0, f1) in enumerate(((0, 3), (1, 2))):
            res = merge([o_buf[k, c, x, ab], fin[k, f0], fin[k, f1]], lat)
            ol[ab, pl.ds(pl.multiple_of(k * 16, 16), 16), :] = jnp.concatenate(
                [o / l for o, _, l in res], axis=0).astype(BF16)

    @pl.loop(0, nch + 3)
    def _(k):
        @pl.when(k < nch)
        def _():
            attend(k)
            d2d_copy(k).start()
            wo_copy(k).start()

        @pl.when((k >= 1) & (k < nch + 1))
        def _():
            pair_stage(k - 1)

        @pl.when((k >= 2) & (k < nch + 2))
        def _():
            mid_stage(k - 2)

        @pl.when(k >= 3)
        def _():
            final_stage(k - 3)

    pltpu.make_async_copy(wuv_hbm, wuv, wuv_sem).wait()
    for ab in range(2):
        ov = jnp.zeros((128, 128), F32)
        src = ol[ab]
        for h in range(8):
            ov += dot(jnp.where(row_h == h, src, jnp.zeros_like(src)), wuv[ab, h * lat:(h + 1) * lat, :])
        ov = dot(to_hb, ov.astype(BF16)).astype(BF16)
        for h in range(8):
            ovb[:, (ab * 8 + h) * 128:(ab * 8 + h + 1) * 128] = ov[h * 16:(h + 1) * 16]
    for j in range(8):
        wo_copy(j).wait()

    yw = dm // n

    def y_copy(d):
        dev = lax.rem(s + d, n)
        return remote(y_send.at[dev], y_recv.at[s], y_s.at[dev], y_r.at[s], dev)

    def y_wait(src):
        return remote(y_send.at[src], y_recv.at[src], y_s.at[src], y_r.at[src], src)

    @pl.loop(1, n + 1)
    def _(d):
        dev = lax.rem(s + d, n)
        y_send[dev] = dot(ovb[...], wo[:, pl.ds(pl.multiple_of(dev * yw, yw), yw)])

        @pl.when(d < n)
        def _():
            y_copy(d).start()

    y = y_send[s]
    for d in range(1, n):
        src = lax.rem(s + d, n)
        y_wait(src).wait_recv()
        y += y_recv[src]
    y += hid[:, pl.ds(pl.multiple_of(s * yw, yw), yw)].astype(F32)
    y_own[...] = y.astype(BF16)

    def g_copy(d):
        dev = lax.rem(s + d, n)
        return remote(y_own, out_all.at[s], g_s.at[dev], g_r.at[s], dev)

    for d in range(1, n):
        g_copy(d).start()
    out_ref[:, pl.ds(pl.multiple_of(s * yw, yw), yw)] = y_own[...]
    for d in range(1, n):
        src = lax.rem(s + d, n)
        remote(y_own, out_all.at[src], g_s.at[src], g_r.at[src], src).wait_recv()
        out_ref[:, pl.ds(pl.multiple_of(src * yw, yw), yw)] = out_all[src]

    for t in range(3):
        ag_done(t)

    @pl.loop(0, nch)
    def _(k):
        d2d_copy(k).wait_send()
        for cp in hop_copies(k) + mid_copies(k):
            cp.wait_send()

    for d in range(1, n):
        y_copy(d).wait_send()
        g_copy(d).wait_send()


def solution(mesh):
    n = mesh.shape['seq']
    row_spec = P('batch', None)
    cache_spec = P('batch', 'seq', None)
    in_specs = (row_spec, P('batch'), cache_spec, cache_spec, P(None, 'seq', None), P(None, 'seq', None),
                P('seq', None, None), P('seq', None, None), P('seq', None, None))

    def mla_step(hidden, lengths, c_kv, k_rope, w_uq, w_qr, w_uk, w_uv, w_o):
        rows, dm = hidden.shape
        t_len, lat = c_kv.shape[1:]
        rope = k_rope.shape[2]
        nh, nope = w_uq.shape[1:]
        vdim = w_uv.shape[2]
        scale = 1.0 / math.sqrt(nope + rope)
        nch, yw, width = rows // RPC, dm // n, RPC * lat + 128
        any_spec = pl.BlockSpec(memory_space=pl.ANY)
        vmem = pl.BlockSpec(memory_space=pltpu.VMEM)
        dma, V = pltpu.SemaphoreType.DMA, pltpu.VMEM
        return pl.pallas_call(
            functools.partial(kernel, n, scale),
            out_shape=jax.ShapeDtypeStruct((rows, dm), BF16),
            in_specs=[pl.BlockSpec(memory_space=pltpu.SMEM), vmem] + [any_spec] * 7,
            out_specs=vmem,
            scratch_shapes=[
                V((rows, dm * 8), BF16), V((SLOTS, DCH, 8, nope), BF16), V((2, 8 * nope, lat), BF16),
                V((2, 8 * lat, vdim), BF16), V((nh * vdim, dm), BF16), V((rows, t_len, lat), BF16),
                V((rows, rope, t_len), BF16), V((128, nope), F32), V((n, 2, 128, lat), BF16),
                V((128, 128), BF16), V((n, 128, 128), BF16), V((RPC, nh * n, lat), BF16),
                V((nch, 2, n // 2, 2, 8, width), F32), V((nch, n // 2, 2, 8, width), F32),
                V((nch, 2, 8, width), F32), V((nch, 4, 8, width), F32), V((2, 128, lat), BF16),
                V((rows, nh * vdim), BF16), V((n, rows, yw), F32), V((n, rows, yw), F32),
                V((rows, yw), BF16), V((n, rows, yw), BF16),
                dma((SLOTS,)), dma((2,)), dma((8,)), dma((rows,)), dma((rows,)), dma(()), dma((8,)),
                dma((3, 7)), dma((3, n)), dma((nch, 7)), dma((nch,)), dma((nch, 2)), dma((nch, 4)),
                dma((n,)), dma((n,)), dma((n,)), dma((n,)),
            ],
            compiler_params=pltpu.CompilerParams(collective_id=0, has_side_effects=True,
                                                 vmem_limit_bytes=67043328),
        )(lengths, hidden, c_kv, jnp.swapaxes(k_rope, 1, 2), w_uq.reshape(dm, 2, nh // 2, nope),
          jnp.transpose(w_qr, (1, 2, 0)).reshape(nh * rope, dm), w_uk.reshape(2, nh // 2 * nope, lat),
          w_uv.reshape(2, nh // 2 * lat, vdim), w_o.reshape(nh * vdim, dm))

    return jax.shard_map(mla_step, mesh=mesh, in_specs=in_specs, out_specs=row_spec, check_vma=False)
```

```python
import functools
import math

import jax
import jax.numpy as jnp
from jax import lax
from jax.experimental import pallas as pl
from jax.experimental.pallas import tpu as pltpu
from jax.sharding import PartitionSpec as P

MESH = pl.DeviceIdType.MESH
F32 = jnp.float32
BF16 = jnp.bfloat16
LOWEST = float(jnp.finfo(jnp.float32).min)
DCH = 512
SLOTS = 4
RPC = 2


def iota(shape, dim):
    return lax.broadcasted_iota(jnp.int32, shape, dim)


def dot(a, b):
    return lax.dot_general(a, b, (((1,), (0,)), ((), ())), preferred_element_type=F32)


def dot_nt(a, b):
    return lax.dot_general(a, b, (((1,), (1,)), ((), ())), preferred_element_type=F32)


def merge(blocks, lat):
    rows = []
    for r in range(RPC):
        base = RPC * lat
        ms = [b[:, base + r:base + r + 1] for b in blocks]
        ls = [b[:, base + RPC + r:base + RPC + r + 1] for b in blocks]
        m = functools.reduce(jnp.maximum, ms)
        ws = [jnp.exp(x - m) for x in ms]
        l = functools.reduce(lambda a, b: a + b, [w * y for w, y in zip(ws, ls)])
        o = functools.reduce(lambda a, b: a + b,
                             [w * b[:, r * lat:(r + 1) * lat] for w, b in zip(ws, blocks)])
        rows.append((o, m, l))
    return rows


def pack_ml(ms, ls, shape):
    lane = iota(shape, 1)
    out = jnp.zeros(shape, F32)
    for r in range(RPC):
        out = jnp.where(lane == r, ms[r], out)
        out = jnp.where(lane == RPC + r, ls[r], out)
    return out


def kernel(n, scale, lens, hid_hbm, c_hbm, k_hbm, wuq_hbm, wqr_hbm, wuk_hbm, wuv_hbm, wo_hbm, out_ref,
           hid, hexp, wbuf, wuk, wuv, wo, cb, kb, acc, q_all, qr_st, qr_all, qrow, o_buf, d2d, mid, fin, ol, ovb,
           y_send, y_pair, y_recv, y_own, out_all,
           hid_sem, w_sem, wuk_sem, wqr_sem, c_sem, k_sem, wuv_sem, wo_sem,
           ag_s, ag_r, rs_s, d2d_r, mid_r, fin_r, yp_s, yp_r, y_s, y_r, g_s, g_r):
    s = lax.axis_index("seq")
    x, c = lax.div(s, 2), lax.rem(s, 2)
    nx = n // 2
    oc = 1 - c
    xr, xl, xo = lax.rem(x + 1, nx), lax.rem(x + nx - 1, nx), lax.rem(x + 2, nx)
    partner, right, left = 2 * x + oc, 2 * xr + c, 2 * xl + c
    rows, dm = hid.shape
    t_len, lat = cb.shape[1], cb.shape[2]
    nheads = 16 * n
    nc = dm // DCH
    nch = rows // RPC

    def remote(src, dst, ssem, rsem, dev):
        return pltpu.make_async_remote_copy(src_ref=src, dst_ref=dst, send_sem=ssem, recv_sem=rsem,
                                            device_id={"seq": dev}, device_id_type=MESH)

    def w_copy(g):
        half, i = lax.div(g, nc), lax.rem(g, nc)
        return pltpu.make_async_copy(wuq_hbm.at[pl.ds(i * DCH, DCH), half], wbuf.at[lax.rem(g, SLOTS)],
                                     w_sem.at[lax.rem(g, SLOTS)])

    def wuk_copy(half):
        return pltpu.make_async_copy(wuk_hbm.at[half], wuk.at[half], wuk_sem.at[half])

    def wqr_copy(j):
        return pltpu.make_async_copy(wqr_hbm.at[pl.ds(j * 128, 128)], wo.at[pl.ds(j * 128, 128)], wqr_sem.at[j])

    def c_copy(b):
        return pltpu.make_async_copy(c_hbm.at[b], cb.at[b], c_sem.at[b])

    def k_copy(b):
        return pltpu.make_async_copy(k_hbm.at[b], kb.at[b], k_sem.at[b])

    def wo_copy(j):
        return pltpu.make_async_copy(wo_hbm.at[pl.ds(j * 256, 256)], wo.at[pl.ds(j * 256, 256)], wo_sem.at[j])

    hid_copy = pltpu.make_async_copy(hid_hbm, hid, hid_sem)
    hid_copy.start()
    for g in range(SLOTS):
        w_copy(jnp.int32(g)).start()
    wuk_copy(0).start()

    barrier = pltpu.get_barrier_semaphore()
    for d in range(1, n):
        pl.semaphore_signal(barrier, inc=1, device_id={"seq": lax.rem(s + d, n)}, device_id_type=MESH)

    hid_copy.wait()
    rep = jnp.where(iota((128, 1024), 0) == lax.div(iota((128, 1024), 1), 8), 1.0, 0.0).astype(BF16)
    ndt = dm // 128
    for g0 in range(0, ndt, 8):
        grp = list(range(g0, min(g0 + 8, ndt)))
        st = jnp.concatenate([hid[:, t * 128:(t + 1) * 128] for t in grp], axis=0)
        ex = dot(st, rep).astype(BF16)
        for i, t in enumerate(grp):
            hexp[:, t * 1024:(t + 1) * 1024] = ex[i * 16:(i + 1) * 16]

    head_mask = jnp.where(lax.div(iota((128, 128), 0), 16) == lax.rem(iota((128, 128), 1), 8), 1.0, 0.0).astype(BF16)
    ri, ci = iota((128, 128), 0), iota((128, 128), 1)
    to_bh = jnp.where(ci == lax.rem(ri, 8) * 16 + lax.div(ri, 8), 1.0, 0.0).astype(BF16)
    to_hb = jnp.where(ci == lax.rem(ri, 16) * 8 + lax.div(ri, 16), 1.0, 0.0).astype(BF16)
    row_h = lax.rem(iota((128, 1), 0), 8)

    opp = 2 * xo + c

    def ag_buf(t, owner):
        return qr_all.at[owner] if t == 4 else q_all.at[owner, t // 2, pl.ds(t % 2 * 64, 64)]

    def ag(t, i, owner, dev):
        return remote(ag_buf(t, owner), ag_buf(t, owner), ag_s.at[t, i], ag_r.at[t, owner], dev)

    def ag_own(half):
        t0, t1 = 2 * half, 2 * half + 1
        for t, i, dev in ((t0, 0, right), (t1, 1, left), (t1, 0, right), (t0, 1, left), (t0, 2, partner),
                          (t1, 2, partner)):
            ag(t, i, s, dev).start()

    def ag_fwd1(half):
        t0, t1 = 2 * half, 2 * half + 1
        ag(t0, 0, left, right).wait_recv()
        ag(t0, 5, left, right).start()
        ag(t0, 3, left, partner).start()
        ag(t1, 1, right, left).wait_recv()
        ag(t1, 5, right, left).start()
        ag(t1, 4, right, partner).start()

    def ag_fwd2(half):
        t0, t1 = 2 * half, 2 * half + 1
        ag(t1, 0, left, right).wait_recv()
        ag(t1, 3, left, partner).start()
        ag(t0, 1, right, left).wait_recv()
        ag(t0, 4, right, partner).start()

    def ag_fwd3(half):
        for t in (2 * half, 2 * half + 1):
            ag(t, 5, opp, right).wait_recv()
            ag(t, 6, opp, partner).start()

    def ag_partner(t):
        for xx in (x, xl, xr, xo):
            ag(t, 2, 2 * xx + oc, partner).wait_recv()

    def ag_done(t):
        for i in range(7):
            ag(t, i, s, partner).wait_send()

    kk = DCH * 8
    def half_step(half):
        acc[...] = jnp.zeros_like(acc)

        @pl.loop(0, nc)
        def _(i):
            g = half * nc + i
            slot = lax.rem(g, SLOTS)
            w_copy(g).wait()
            wv = wbuf[slot].reshape(kk, 128)
            part = acc[...]
            for q0 in range(0, kk, 512):
                hx = hexp[:, pl.ds(pl.multiple_of(i * kk + q0, 512), 512)]
                lhs = jnp.concatenate([hx] * 8, axis=0) * jnp.concatenate([head_mask] * 4, axis=1)
                part += dot(lhs, wv[q0:q0 + 512])
            acc[...] = part

            @pl.when(g + SLOTS < 2 * nc)
            def _():
                w_copy(g + SLOTS).start()

            @pl.when(g >= 2 * nc - SLOTS)
            def _():
                for e in range(8 // SLOTS):
                    wqr_copy((g - (2 * nc - SLOTS)) * (8 // SLOTS) + e).start()

            if half == 0:
                @pl.when(i == 1)
                def _():
                    wuk_copy(1).start()
            else:
                @pl.when(i == nc - 1)
                def _():
                    ag_fwd1(0)

        qn = dot(to_bh, acc[...].astype(BF16)).astype(BF16)
        wuk_copy(half).wait()
        ql = jnp.zeros((128, lat), F32)
        for h in range(8):
            ql += dot(jnp.where(row_h == h, qn, jnp.zeros_like(qn)), wuk[half, h * 128:(h + 1) * 128, :])
        q_all[s, half] = ql.astype(BF16)
        if half == 0:
            pl.semaphore_wait(barrier, n - 1)
        ag_own(half)

    half_step(0)
    half_step(1)

    @pl.loop(0, 8)
    def _(j):
        wqr_copy(j).wait()
        qr = dot_nt(hid[...], wo[pl.ds(pl.multiple_of(j * 128, 128), 128), :])
        qr_st[pl.ds(pl.multiple_of(j * 16, 16), 16), :] = qr.astype(BF16)
        for r in range(2):
            b = 2 * j + r
            c_copy(b).start()
            k_copy(b).start()

        @pl.when(j == 2)
        def _():
            ag_fwd2(0)

        @pl.when(j == 6)
        def _():
            ag_fwd3(0)

    qr_all[s] = dot(to_bh, qr_st[...]).astype(BF16)
    for i, dev in ((0, right), (1, left), (5, opp), (2, partner)):
        ag(4, i, s, dev).start()
    pltpu.make_async_copy(wuv_hbm, wuv, wuv_sem).start()
    ag_fwd1(1)
    ag_fwd2(1)
    for i, owner in ((3, left), (4, right), (6, opp)):
        ag(4, 0, owner, right).wait_recv()
        ag(4, i, owner, partner).start()
    ag_fwd3(1)
    for t in range(5):
        ag_partner(t)

    dup = jnp.where(lax.div(iota((128, 64), 0), 2) == iota((128, 64), 1), 1.0, 0.0).astype(BF16)
    rope_mask = jnp.where(lax.rem(iota((128, 128), 0), 2) == lax.div(iota((128, 128), 1), 64), 1.0, 0.0)
    pos = s * t_len + iota((1, t_len), 1)
    width = RPC * lat + 128

    def attend(k):
        k16 = pl.ds(pl.multiple_of(k * 16, 16), 16)
        for p in range(n):
            qa = q_all[p, 0, k16, :].astype(F32)
            qb = q_all[p, 1, k16, :].astype(F32)
            for r in range(RPC):
                qrow[r, p * 16:(p + 1) * 16, :] = jnp.concatenate(
                    [qa[r * 8:(r + 1) * 8], qb[r * 8:(r + 1) * 8]], axis=0).astype(BF16)
        mls = []
        for r in range(RPC):
            b = k * RPC + r
            c_copy(b).wait()
            k_copy(b).wait()
            pairs = jnp.concatenate(
                [qr_all[p, k16, :].astype(F32)[r * 8:(r + 1) * 8] for p in range(n)], axis=0).astype(BF16)
            qr = (dot(dup, pairs) * rope_mask).astype(BF16)
            keys = kb[b]
            sc = dot_nt(qrow[r], cb[b]) + dot(qr, jnp.concatenate([keys, keys], axis=0))
            sc = jnp.where(pos < lens[b], sc * scale, -jnp.inf)
            m = jnp.maximum(jnp.max(sc, axis=1, keepdims=True), LOWEST)
            pw = jnp.exp(sc - m)
            l = jnp.sum(pw, axis=1, keepdims=True)
            o = dot(pw.astype(BF16), cb[b])
            for p in range(n):
                for ab in range(2):
                    h0 = p * 16 + ab * 8
                    o_buf[k, p % 2, p // 2, ab, :, r * lat:(r + 1) * lat] = o[h0:h0 + 8]
            mls.append((m, l))
        ml = pack_ml([a for a, _ in mls], [a for _, a in mls], (nheads, 128))
        for p in range(n):
            for ab in range(2):
                h0 = p * 16 + ab * 8
                o_buf[k, p % 2, p // 2, ab, :, RPC * lat:] = ml[h0:h0 + 8]

    def d2d_copy(k):
        return remote(o_buf.at[k, oc], d2d.at[k], rs_s.at[k, 0], d2d_r.at[k], partner)

    def hop_copies(k):
        return [
            remote(o_buf.at[k, c, xo, 1], mid.at[k, 0], rs_s.at[k, 1], mid_r.at[k, 0], right),
            remote(o_buf.at[k, c, xo, 0], mid.at[k, 1], rs_s.at[k, 2], mid_r.at[k, 1], left),
            remote(o_buf.at[k, c, xr, 0], fin.at[k, 0], rs_s.at[k, 3], fin_r.at[k, 0], right),
            remote(o_buf.at[k, c, xl, 1], fin.at[k, 1], rs_s.at[k, 4], fin_r.at[k, 1], left),
        ]

    def mid_copies(k):
        return [
            remote(o_buf.at[k, c, xr, 1], fin.at[k, 2], rs_s.at[k, 5], fin_r.at[k, 2], right),
            remote(o_buf.at[k, c, xl, 0], fin.at[k, 3], rs_s.at[k, 6], fin_r.at[k, 3], left),
        ]

    def store_merged(k, xx, ab, other):
        ref = o_buf.at[k, c, xx, ab]
        res = merge([ref[...], other], lat)
        for r in range(RPC):
            ref[:, r * lat:(r + 1) * lat] = res[r][0]
        ref[:, RPC * lat:] = pack_ml([a[1] for a in res], [a[2] for a in res], (8, 128))

    def pair_stage(k):
        d2d_copy(k).wait_recv()
        for xx in range(nx):
            for ab in range(2):
                store_merged(k, xx, ab, d2d[k, xx, ab])
        for cp in hop_copies(k):
            cp.start()

    def mid_stage(k):
        hops, mids = hop_copies(k), mid_copies(k)
        hops[0].wait_recv()
        store_merged(k, xr, 1, mid[k, 0])
        mids[0].start()
        hops[1].wait_recv()
        store_merged(k, xl, 0, mid[k, 1])
        mids[1].start()

    def final_stage(k):
        hops, mids = hop_copies(k), mid_copies(k)
        hops[2].wait_recv()
        hops[3].wait_recv()
        mids[0].wait_recv()
        mids[1].wait_recv()
        for ab, (f0, f1) in enumerate(((0, 3), (1, 2))):
            res = merge([o_buf[k, c, x, ab], fin[k, f0], fin[k, f1]], lat)
            ol[ab, pl.ds(pl.multiple_of(k * 16, 16), 16), :] = jnp.concatenate(
                [o / l for o, _, l in res], axis=0).astype(BF16)

    @pl.loop(0, nch + 5)
    def _(k):
        @pl.when(k < nch)
        def _():
            attend(k)
            d2d_copy(k).start()
            wo_copy(k).start()

        @pl.when((k >= 1) & (k < nch + 1))
        def _():
            pair_stage(k - 1)

        @pl.when((k >= 3) & (k < nch + 3))
        def _():
            mid_stage(k - 3)

        @pl.when(k >= 5)
        def _():
            final_stage(k - 5)

    pltpu.make_async_copy(wuv_hbm, wuv, wuv_sem).wait()
    for ab in range(2):
        ov = jnp.zeros((128, 128), F32)
        src = ol[ab]
        for h in range(8):
            ov += dot(jnp.where(row_h == h, src, jnp.zeros_like(src)), wuv[ab, h * lat:(h + 1) * lat, :])
        ov = dot(to_hb, ov.astype(BF16)).astype(BF16)
        for h in range(8):
            ovb[:, (ab * 8 + h) * 128:(ab * 8 + h + 1) * 128] = ov[h * 16:(h + 1) * 16]
    for j in range(8):
        wo_copy(j).wait()

    yw = dm // n

    def y_block(p):
        return dot(ovb[...], wo[:, pl.ds(pl.multiple_of(p * yw, yw), yw)])

    def yp_copy(xx):
        return remote(y_send.at[2 * xx + oc], y_pair.at[xx], yp_s.at[xx], yp_r.at[xx], partner)

    def y_copy(xx):
        return remote(y_send.at[2 * xx + c], y_recv.at[x], y_s.at[xx], y_r.at[x], 2 * xx + c)

    @pl.loop(0, nx)
    def _(i):
        xx = lax.rem(x + nx - 1 - i, nx)
        y_send[2 * xx + oc] = y_block(2 * xx + oc)
        yp_copy(xx).start()

    @pl.loop(0, nx)
    def _(i):
        xx = lax.rem(x + nx - 1 - i, nx)
        blk = y_block(2 * xx + c)
        yp_copy(xx).wait_recv()
        y_send[2 * xx + c] = blk + y_pair[xx]

        @pl.when(i < nx - 1)
        def _():
            y_copy(xx).start()

    y = y_send[s]
    for xx in (xr, xl, xo):
        remote(y_send.at[s], y_recv.at[xx], y_s.at[xx], y_r.at[xx], right).wait_recv()
        y += y_recv[xx]
    y += hid[:, pl.ds(pl.multiple_of(s * yw, yw), yw)].astype(F32)
    y_own[...] = y.astype(BF16)

    def g_copy(d):
        dev = lax.rem(s + d, n)
        return remote(y_own, out_all.at[s], g_s.at[dev], g_r.at[s], dev)

    for d in range(1, n):
        g_copy(d).start()
    out_ref[:, pl.ds(pl.multiple_of(s * yw, yw), yw)] = y_own[...]
    for d in range(1, n):
        src = lax.rem(s + d, n)
        remote(y_own, out_all.at[src], g_s.at[src], g_r.at[src], src).wait_recv()
        out_ref[:, pl.ds(pl.multiple_of(src * yw, yw), yw)] = out_all[src]

    for t in range(5):
        ag_done(t)

    @pl.loop(0, nch)
    def _(k):
        d2d_copy(k).wait_send()
        for cp in hop_copies(k) + mid_copies(k):
            cp.wait_send()

    for xx in range(nx):
        yp_copy(xx).wait_send()
    for xx in (xr, xl, xo):
        y_copy(xx).wait_send()
    for d in range(1, n):
        g_copy(d).wait_send()


def solution(mesh):
    n = mesh.shape['seq']
    row_spec = P('batch', None)
    cache_spec = P('batch', 'seq', None)
    in_specs = (row_spec, P('batch'), cache_spec, cache_spec, P(None, 'seq', None), P(None, 'seq', None),
                P('seq', None, None), P('seq', None, None), P('seq', None, None))

    def mla_step(hidden, lengths, c_kv, k_rope, w_uq, w_qr, w_uk, w_uv, w_o):
        rows, dm = hidden.shape
        t_len, lat = c_kv.shape[1:]
        rope = k_rope.shape[2]
        nh, nope = w_uq.shape[1:]
        vdim = w_uv.shape[2]
        scale = 1.0 / math.sqrt(nope + rope)
        nch, yw, width = rows // RPC, dm // n, RPC * lat + 128
        any_spec = pl.BlockSpec(memory_space=pl.ANY)
        vmem = pl.BlockSpec(memory_space=pltpu.VMEM)
        dma, V = pltpu.SemaphoreType.DMA, pltpu.VMEM
        return pl.pallas_call(
            functools.partial(kernel, n, scale),
            out_shape=jax.ShapeDtypeStruct((rows, dm), BF16),
            in_specs=[pl.BlockSpec(memory_space=pltpu.SMEM)] + [any_spec] * 8,
            out_specs=vmem,
            scratch_shapes=[
                V((rows, dm), BF16), V((rows, dm * 8), BF16), V((SLOTS, DCH, 8, nope), BF16), V((2, 8 * nope, lat), BF16),
                V((2, 8 * lat, vdim), BF16), V((nh * vdim, dm), BF16), V((rows, t_len, lat), BF16),
                V((rows, rope, t_len), BF16), V((128, nope), F32), V((n, 2, 128, lat), BF16),
                V((128, 128), BF16), V((n, 128, 128), BF16), V((RPC, nh * n, lat), BF16),
                V((nch, 2, n // 2, 2, 8, width), F32), V((nch, n // 2, 2, 8, width), F32),
                V((nch, 2, 8, width), F32), V((nch, 4, 8, width), F32), V((2, 128, lat), BF16),
                V((rows, nh * vdim), BF16), V((n, rows, yw), F32), V((n // 2, rows, yw), F32), V((n // 2, rows, yw), F32),
                V((rows, yw), BF16), V((n, rows, yw), BF16),
                dma(()), dma((SLOTS,)), dma((2,)), dma((8,)), dma((rows,)), dma((rows,)), dma(()), dma((8,)),
                dma((5, 7)), dma((5, n)), dma((nch, 7)), dma((nch,)), dma((nch, 2)), dma((nch, 4)),
                dma((n // 2,)), dma((n // 2,)), dma((n // 2,)), dma((n // 2,)), dma((n,)), dma((n,)),
            ],
            compiler_params=pltpu.CompilerParams(collective_id=0, has_side_effects=True,
                                                 vmem_limit_bytes=67043328),
        )(lengths, hidden, c_kv, jnp.swapaxes(k_rope, 1, 2), w_uq.reshape(dm, 2, nh // 2, nope),
          jnp.transpose(w_qr, (1, 2, 0)).reshape(nh * rope, dm), w_uk.reshape(2, nh // 2 * nope, lat),
          w_uv.reshape(2, nh // 2 * lat, vdim), w_o.reshape(nh * vdim, dm))

    return jax.shard_map(mla_step, mesh=mesh, in_specs=in_specs, out_specs=row_spec, check_vma=False)
```

```python
import functools
import math

import jax
import jax.numpy as jnp
from jax import lax
from jax.experimental import pallas as pl
from jax.experimental.pallas import tpu as pltpu
from jax.sharding import PartitionSpec as P

MESH = pl.DeviceIdType.MESH
F32 = jnp.float32
BF16 = jnp.bfloat16
LOWEST = float(jnp.finfo(jnp.float32).min)
DCH = 512
SLOTS = 4
KST = 1024
RPC = 2


def iota(shape, dim):
    return lax.broadcasted_iota(jnp.int32, shape, dim)


def dot(a, b):
    return lax.dot_general(a, b, (((1,), (0,)), ((), ())), preferred_element_type=F32)


def dot_nt(a, b):
    return lax.dot_general(a, b, (((1,), (1,)), ((), ())), preferred_element_type=F32)


def merge(blocks, lat):
    rows = []
    for r in range(RPC):
        base = RPC * lat
        ms = [b[:, base + r:base + r + 1] for b in blocks]
        ls = [b[:, base + RPC + r:base + RPC + r + 1] for b in blocks]
        m = functools.reduce(jnp.maximum, ms)
        ws = [jnp.exp(x - m) for x in ms]
        l = functools.reduce(lambda a, b: a + b, [w * y for w, y in zip(ws, ls)])
        o = functools.reduce(lambda a, b: a + b,
                             [w * b[:, r * lat:(r + 1) * lat] for w, b in zip(ws, blocks)])
        rows.append((o, m, l))
    return rows


def pack_ml(ms, ls, shape):
    lane = iota(shape, 1)
    out = jnp.zeros(shape, F32)
    for r in range(RPC):
        out = jnp.where(lane == r, ms[r], out)
        out = jnp.where(lane == RPC + r, ls[r], out)
    return out


def kernel(n, scale, lens, hid_hbm, c_hbm, k_hbm, wuq_hbm, wqr_hbm, wuk_hbm, wuv_hbm, wo_hbm, out_ref,
           hid, hexp, wbuf, wuk, wuv, wo, cb, kb, acc, q_all, qr_st, qr_all, qrow, o_buf, d2d, mid, fin, ol, ovb,
           y_send, y_pair, y_recv, y_own, out_all,
           hid_sem, w_sem, wuk_sem, wqr_sem, c_sem, k_sem, wuv_sem, wo_sem,
           ag_s, ag_r, d2d_s, rs_s, d2d_r, mid_r, fin_r, yp_s, yp_r, y_s, y_r, g_s, g_r):
    s = lax.axis_index("seq")
    x, c = lax.div(s, 2), lax.rem(s, 2)
    nx = n // 2
    oc = 1 - c
    xr, xl, xo = lax.rem(x + 1, nx), lax.rem(x + nx - 1, nx), lax.rem(x + 2, nx)
    partner, right, left = 2 * x + oc, 2 * xr + c, 2 * xl + c
    rows, dm = hid.shape
    t_len, lat = cb.shape[1], cb.shape[2]
    nheads = 16 * n
    nc = dm // DCH
    nch = rows // RPC

    def remote(src, dst, ssem, rsem, dev):
        return pltpu.make_async_remote_copy(src_ref=src, dst_ref=dst, send_sem=ssem, recv_sem=rsem,
                                            device_id={"seq": dev}, device_id_type=MESH)

    def w_copy(g):
        half, i = lax.div(g, nc), lax.rem(g, nc)
        return pltpu.make_async_copy(wuq_hbm.at[pl.ds(i * DCH, DCH), half], wbuf.at[lax.rem(g, SLOTS)],
                                     w_sem.at[lax.rem(g, SLOTS)])

    def wuk_copy(half):
        return pltpu.make_async_copy(wuk_hbm.at[half], wuk.at[half], wuk_sem.at[half])

    def wqr_copy(j):
        return pltpu.make_async_copy(wqr_hbm.at[pl.ds(j * 128, 128)], wo.at[pl.ds(j * 128, 128)], wqr_sem.at[j])

    def c_copy(b):
        return pltpu.make_async_copy(c_hbm.at[b], cb.at[b], c_sem.at[b])

    def k_copy(b):
        return pltpu.make_async_copy(k_hbm.at[b], kb.at[b], k_sem.at[b])

    def wo_copy(j):
        return pltpu.make_async_copy(wo_hbm.at[pl.ds(j * 256, 256)], wo.at[pl.ds(j * 256, 256)], wo_sem.at[j])

    hid_copy = pltpu.make_async_copy(hid_hbm, hid, hid_sem)
    hid_copy.start()
    for g in range(SLOTS):
        w_copy(jnp.int32(g)).start()
    wuk_copy(0).start()

    barrier = pltpu.get_barrier_semaphore()
    for d in range(1, n):
        pl.semaphore_signal(barrier, inc=1, device_id={"seq": lax.rem(s + d, n)}, device_id_type=MESH)

    hid_copy.wait()
    rep = jnp.where(iota((128, 1024), 0) == lax.div(iota((128, 1024), 1), 8), 1.0, 0.0).astype(BF16)
    ndt = dm // 128
    for g0 in range(0, ndt, 8):
        grp = list(range(g0, min(g0 + 8, ndt)))
        st = jnp.concatenate([hid[:, t * 128:(t + 1) * 128] for t in grp], axis=0)
        ex = dot(st, rep).astype(BF16)
        for i, t in enumerate(grp):
            hexp[:, t * 1024:(t + 1) * 1024] = ex[i * 16:(i + 1) * 16]

    head_mask = jnp.where(lax.div(iota((128, 128), 0), 16) == lax.rem(iota((128, 128), 1), 8), 1.0, 0.0).astype(BF16)
    ri, ci = iota((128, 128), 0), iota((128, 128), 1)
    to_bh = jnp.where(ci == lax.rem(ri, 8) * 16 + lax.div(ri, 8), 1.0, 0.0).astype(BF16)
    to_hb = jnp.where(ci == lax.rem(ri, 16) * 8 + lax.div(ri, 16), 1.0, 0.0).astype(BF16)
    row_h = lax.rem(iota((128, 1), 0), 8)

    opp = 2 * xo + c

    def ag_buf(t, owner):
        return qr_all.at[owner] if t == 4 else q_all.at[owner, t // 2, pl.ds(t % 2 * 64, 64)]

    def ag(t, i, owner, dev):
        return remote(ag_buf(t, owner), ag_buf(t, owner), ag_s.at[t, i], ag_r.at[t, owner], dev)

    def ag_own(half):
        t0, t1 = 2 * half, 2 * half + 1
        for t, i, dev in ((t0, 0, right), (t1, 1, left), (t1, 0, right), (t0, 1, left), (t0, 2, partner),
                          (t1, 2, partner)):
            ag(t, i, s, dev).start()

    def ag_fwd1(half):
        t0, t1 = 2 * half, 2 * half + 1
        ag(t0, 0, left, right).wait_recv()
        ag(t0, 5, left, right).start()
        ag(t0, 3, left, partner).start()
        ag(t1, 1, right, left).wait_recv()
        ag(t1, 5, right, left).start()
        ag(t1, 4, right, partner).start()

    def ag_fwd2(half):
        t0, t1 = 2 * half, 2 * half + 1
        ag(t1, 0, left, right).wait_recv()
        ag(t1, 3, left, partner).start()
        ag(t0, 1, right, left).wait_recv()
        ag(t0, 4, right, partner).start()

    def ag_fwd3(half):
        for t in (2 * half, 2 * half + 1):
            ag(t, 5, opp, right).wait_recv()
            ag(t, 6, opp, partner).start()

    def ag_partner(t):
        for xx in (x, xl, xr, xo):
            ag(t, 2, 2 * xx + oc, partner).wait_recv()

    def ag_done(t):
        for i in range(7):
            ag(t, i, s, partner).wait_send()

    kk = DCH * 8
    def half_step(half):
        acc[...] = jnp.zeros_like(acc)

        @pl.loop(0, nc // 2)
        def _(i2):
            part = acc[...]
            for u in range(2):
                i = 2 * i2 + u
                g = half * nc + i
                w_copy(g).wait()
                wv = wbuf[lax.rem(g, SLOTS)].reshape(kk, 128)
                for q0 in range(0, kk, KST):
                    hx = hexp[:, pl.ds(pl.multiple_of(i * kk + q0, KST), KST)]
                    lhs = jnp.concatenate([hx] * 8, axis=0) * jnp.concatenate([head_mask] * (KST // 128), axis=1)
                    part += dot(lhs, wv[q0:q0 + KST])
            acc[...] = part
            g0 = half * nc + 2 * i2

            @pl.when(g0 + SLOTS < 2 * nc)
            def _():
                w_copy(g0 + SLOTS).start()
                w_copy(g0 + SLOTS + 1).start()

            @pl.when(g0 >= 2 * nc - SLOTS)
            def _():
                for e in range(16 // SLOTS):
                    wqr_copy((g0 - (2 * nc - SLOTS)) * (8 // SLOTS) + e).start()

            if half == 0:
                @pl.when(i2 == 0)
                def _():
                    wuk_copy(1).start()
            else:
                @pl.when(i2 == nc // 2 - 1)
                def _():
                    ag_fwd1(0)

        qn = dot(to_bh, acc[...].astype(BF16)).astype(BF16)
        wuk_copy(half).wait()
        ql = jnp.zeros((128, lat), F32)
        for h in range(8):
            ql += dot(jnp.where(row_h == h, qn, jnp.zeros_like(qn)), wuk[half, h * 128:(h + 1) * 128, :])
        q_all[s, half] = ql.astype(BF16)
        if half == 0:
            pl.semaphore_wait(barrier, n - 1)
        ag_own(half)

    half_step(0)
    half_step(1)

    @pl.loop(0, 8)
    def _(j):
        wqr_copy(j).wait()
        qr = dot_nt(wo[pl.ds(pl.multiple_of(j * 128, 128), 128), :], hid[...])
        qr_st[pl.ds(pl.multiple_of(j * 16, 16), 16), :] = qr.T.astype(BF16)
        for r in range(2):
            b = 2 * j + r
            c_copy(b).start()
            k_copy(b).start()

        @pl.when(j == 2)
        def _():
            ag_fwd2(0)

        @pl.when(j == 6)
        def _():
            ag_fwd3(0)

    qr_all[s] = dot(to_bh, qr_st[...]).astype(BF16)
    for i, dev in ((0, right), (1, left), (5, opp), (2, partner)):
        ag(4, i, s, dev).start()
    pltpu.make_async_copy(wuv_hbm, wuv, wuv_sem).start()
    ag_fwd1(1)
    ag_fwd2(1)
    for i, owner in ((3, left), (4, right), (6, opp)):
        ag(4, 0, owner, right).wait_recv()
        ag(4, i, owner, partner).start()
    ag_fwd3(1)
    for t in range(5):
        ag_partner(t)

    dup = jnp.where(lax.div(iota((128, 64), 0), 2) == iota((128, 64), 1), 1.0, 0.0).astype(BF16)
    rope_mask = jnp.where(lax.rem(iota((128, 128), 0), 2) == lax.div(iota((128, 128), 1), 64), 1.0, 0.0)
    pos = s * t_len + iota((1, t_len), 1)
    width = RPC * lat + 128

    def attend(k):
        k16 = pl.ds(pl.multiple_of(k * 16, 16), 16)
        for p in range(n):
            qa = q_all[p, 0, k16, :].astype(F32)
            qb = q_all[p, 1, k16, :].astype(F32)
            for r in range(RPC):
                qrow[r, p * 16:(p + 1) * 16, :] = jnp.concatenate(
                    [qa[r * 8:(r + 1) * 8], qb[r * 8:(r + 1) * 8]], axis=0).astype(BF16)
        mls = []
        for r in range(RPC):
            b = k * RPC + r
            c_copy(b).wait()
            k_copy(b).wait()
            pairs = jnp.concatenate(
                [qr_all[p, k16, :].astype(F32)[r * 8:(r + 1) * 8] for p in range(n)], axis=0).astype(BF16)
            qr = (dot(dup, pairs) * rope_mask).astype(BF16)
            keys = kb[b]
            sc = dot_nt(qrow[r], cb[b]) + dot(qr, jnp.concatenate([keys, keys], axis=0))
            sc = jnp.where(pos < lens[b], sc * scale, -jnp.inf)
            m = jnp.maximum(jnp.max(sc, axis=1, keepdims=True), LOWEST)
            pw = jnp.exp(sc - m)
            l = jnp.sum(pw, axis=1, keepdims=True)
            o = dot(pw.astype(BF16), cb[b])
            for p in range(n):
                for ab in range(2):
                    h0 = p * 16 + ab * 8
                    o_buf[k, p % 2, p // 2, ab, :, r * lat:(r + 1) * lat] = o[h0:h0 + 8]
            mls.append((m, l))
        ml = pack_ml([a for a, _ in mls], [a for _, a in mls], (nheads, 128))
        for p in range(n):
            for ab in range(2):
                h0 = p * 16 + ab * 8
                o_buf[k, p % 2, p // 2, ab, :, RPC * lat:] = ml[h0:h0 + 8]

    def d2d_copy(k):
        return remote(o_buf.at[k, oc], d2d.at[k], d2d_s.at[k], d2d_r.at[k], partner)

    def sides(k):
        turn = 1 - 2 * lax.rem(k, 2)
        return lax.rem(x + nx + turn, nx), lax.rem(x + nx - turn, nx)

    def far_copy(ab, k):
        xp, _ = sides(k)
        return remote(o_buf.at[k, c, xo, ab], mid.at[k, ab], rs_s.at[k, ab, 0], mid_r.at[k, ab], 2 * xp + c)

    def near_copy(ab, k):
        _, xq = sides(k)
        return remote(o_buf.at[k, c, xq, ab], fin.at[k, ab, 0], rs_s.at[k, ab, 1], fin_r.at[k, ab, 0], 2 * xq + c)

    def mid_copy(ab, k):
        xp, _ = sides(k)
        return remote(o_buf.at[k, c, xp, ab], fin.at[k, ab, 1], rs_s.at[k, ab, 2], fin_r.at[k, ab, 1], 2 * xp + c)

    def store_merged(k, xx, ab, other):
        ref = o_buf.at[k, c, xx, ab]
        res = merge([ref[...], other], lat)
        for r in range(RPC):
            ref[:, r * lat:(r + 1) * lat] = res[r][0]
        ref[:, RPC * lat:] = pack_ml([a[1] for a in res], [a[2] for a in res], (8, 128))

    def pair_stage(k):
        d2d_copy(k).wait_recv()
        for ab in range(2):
            for xx in range(nx):
                store_merged(k, xx, ab, d2d[k, xx, ab])

    def hop(ab, k):
        far_copy(ab, k).start()
        near_copy(ab, k).start()

    def mid_stage(ab, k):
        xp, _ = sides(k)
        far_copy(ab, k).wait_recv()
        store_merged(k, xp, ab, mid[k, ab])
        mid_copy(ab, k).start()

    def final_stage(ab, k):
        near_copy(ab, k).wait_recv()
        mid_copy(ab, k).wait_recv()
        res = merge([o_buf[k, c, x, ab], fin[k, ab, 0], fin[k, ab, 1]], lat)
        ol[ab, pl.ds(pl.multiple_of(k * 16, 16), 16), :] = jnp.concatenate(
            [o / l for o, _, l in res], axis=0).astype(BF16)

    early2 = nch // 2

    @pl.loop(0, nch + 1)
    def _(k):
        @pl.when(k < nch)
        def _():
            attend(k)
            d2d_copy(k).start()
            wo_copy(k).start()

        @pl.when(k >= 1)
        def _():
            pair_stage(k - 1)
            hop(0, k - 1)

            @pl.when(lax.rem(k, 2) == 1)
            def _():
                @pl.when(k < nch)
                def _():
                    hop(1, lax.div(k - 1, 2))

        @pl.when(k >= 3)
        def _():
            mid_stage(0, k - 3)

            @pl.when(lax.rem(k, 2) == 1)
            def _():
                mid_stage(1, lax.div(k - 3, 2))

        @pl.when(k >= 5)
        def _():
            final_stage(0, k - 5)

    @pl.loop(early2, nch)
    def _(k):
        hop(1, k)

    @pl.loop(nch - 2, nch)
    def _(k):
        mid_stage(0, k)

    mid_stage(1, early2 - 1)

    @pl.loop(nch - 4, nch)
    def _(k):
        final_stage(0, k)

    pltpu.make_async_copy(wuv_hbm, wuv, wuv_sem).wait()
    hrows = wo.shape[0] // 2
    yw = dm // n

    def values(ab):
        ov = jnp.zeros((128, 128), F32)
        src = ol[ab]
        for h in range(8):
            ov += dot(jnp.where(row_h == h, src, jnp.zeros_like(src)), wuv[ab, h * lat:(h + 1) * lat, :])
        ov = dot(to_hb, ov.astype(BF16)).astype(BF16)
        for h in range(8):
            ovb[ab, :, h * 128:(h + 1) * 128] = ov[h * 16:(h + 1) * 16]

    def y_block(ab, p):
        return dot(ovb[ab], wo[ab * hrows:(ab + 1) * hrows, pl.ds(pl.multiple_of(p * yw, yw), yw)])

    values(0)
    for j in range(8):
        wo_copy(j).wait()

    @pl.loop(0, n)
    def _(p):
        y_send[p] = y_block(0, p)

        @pl.when(p >= n - (nch - early2))
        def _():
            mid_stage(1, p - (n - nch))

    @pl.loop(0, nch)
    def _(k):
        final_stage(1, k)

    values(1)

    def yp_copy(xx):
        return remote(y_send.at[2 * xx + oc], y_pair.at[xx], yp_s.at[xx], yp_r.at[xx], partner)

    def y_copy(xx):
        return remote(y_send.at[2 * xx + c], y_recv.at[x], y_s.at[xx], y_r.at[x], 2 * xx + c)

    @pl.loop(0, nx)
    def _(i):
        xx = lax.rem(x + nx - 1 - i, nx)
        y_send[2 * xx + oc] += y_block(1, 2 * xx + oc)
        yp_copy(xx).start()

    @pl.loop(0, nx)
    def _(i):
        xx = lax.rem(x + nx - 1 - i, nx)
        blk = y_send[2 * xx + c] + y_block(1, 2 * xx + c)
        yp_copy(xx).wait_recv()
        y_send[2 * xx + c] = blk + y_pair[xx]

        @pl.when(i < nx - 1)
        def _():
            y_copy(xx).start()

    y = y_send[s]
    for xx in (xr, xl, xo):
        remote(y_send.at[s], y_recv.at[xx], y_s.at[xx], y_r.at[xx], right).wait_recv()
        y += y_recv[xx]
    y += hid[:, pl.ds(pl.multiple_of(s * yw, yw), yw)].astype(F32)
    y_own[...] = y.astype(BF16)

    def g_copy(d):
        dev = lax.rem(s + d, n)
        return remote(y_own, out_all.at[s], g_s.at[dev], g_r.at[s], dev)

    for d in range(1, n):
        g_copy(d).start()
    out_ref[:, pl.ds(pl.multiple_of(s * yw, yw), yw)] = y_own[...]
    for d in range(1, n):
        src = lax.rem(s + d, n)
        remote(y_own, out_all.at[src], g_s.at[src], g_r.at[src], src).wait_recv()
        out_ref[:, pl.ds(pl.multiple_of(src * yw, yw), yw)] = out_all[src]

    for t in range(5):
        ag_done(t)

    @pl.loop(0, nch)
    def _(k):
        d2d_copy(k).wait_send()
        for ab in range(2):
            for cp in (far_copy(ab, k), near_copy(ab, k), mid_copy(ab, k)):
                cp.wait_send()

    for xx in range(nx):
        yp_copy(xx).wait_send()
    for xx in (xr, xl, xo):
        y_copy(xx).wait_send()
    for d in range(1, n):
        g_copy(d).wait_send()


def solution(mesh):
    n = mesh.shape['seq']
    row_spec = P('batch', None)
    cache_spec = P('batch', 'seq', None)
    in_specs = (row_spec, P('batch'), cache_spec, cache_spec, P(None, 'seq', None), P(None, 'seq', None),
                P('seq', None, None), P('seq', None, None), P('seq', None, None))

    def mla_step(hidden, lengths, c_kv, k_rope, w_uq, w_qr, w_uk, w_uv, w_o):
        rows, dm = hidden.shape
        t_len, lat = c_kv.shape[1:]
        rope = k_rope.shape[2]
        nh, nope = w_uq.shape[1:]
        vdim = w_uv.shape[2]
        scale = 1.0 / math.sqrt(nope + rope)
        nch, yw, width = rows // RPC, dm // n, RPC * lat + 128
        any_spec = pl.BlockSpec(memory_space=pl.ANY)
        vmem = pl.BlockSpec(memory_space=pltpu.VMEM)
        dma, V = pltpu.SemaphoreType.DMA, pltpu.VMEM
        return pl.pallas_call(
            functools.partial(kernel, n, scale),
            out_shape=jax.ShapeDtypeStruct((rows, dm), BF16),
            in_specs=[pl.BlockSpec(memory_space=pltpu.SMEM)] + [any_spec] * 8,
            out_specs=vmem,
            scratch_shapes=[
                V((rows, dm), BF16), V((rows, dm * 8), BF16), V((SLOTS, DCH, 8, nope), BF16), V((2, 8 * nope, lat), BF16),
                V((2, 8 * lat, vdim), BF16), V((nh * vdim, dm), BF16), V((rows, t_len, lat), BF16),
                V((rows, rope, t_len), BF16), V((128, nope), F32), V((n, 2, 128, lat), BF16),
                V((128, 128), BF16), V((n, 128, 128), BF16), V((RPC, nh * n, lat), BF16),
                V((nch, 2, n // 2, 2, 8, width), F32), V((nch, n // 2, 2, 8, width), F32),
                V((nch, 2, 8, width), F32), V((nch, 2, 2, 8, width), F32), V((2, 128, lat), BF16),
                V((2, rows, nh * vdim // 2), BF16), V((n, rows, yw), F32), V((n // 2, rows, yw), F32), V((n // 2, rows, yw), F32),
                V((rows, yw), BF16), V((n, rows, yw), BF16),
                dma(()), dma((SLOTS,)), dma((2,)), dma((8,)), dma((rows,)), dma((rows,)), dma(()), dma((8,)),
                dma((5, 7)), dma((5, n)), dma((nch,)), dma((nch, 2, 3)), dma((nch,)), dma((nch, 2)), dma((nch, 2, 2)),
                dma((n // 2,)), dma((n // 2,)), dma((n // 2,)), dma((n // 2,)), dma((n,)), dma((n,)),
            ],
            compiler_params=pltpu.CompilerParams(collective_id=0, has_side_effects=True,
                                                 vmem_limit_bytes=67043328),
        )(lengths, hidden, c_kv, jnp.swapaxes(k_rope, 1, 2), w_uq.reshape(dm, 2, nh // 2, nope),
          jnp.transpose(w_qr, (1, 2, 0)).reshape(nh * rope, dm), w_uk.reshape(2, nh // 2 * nope, lat),
          w_uv.reshape(2, nh // 2 * lat, vdim), w_o.reshape(nh * vdim, dm))

    return jax.shard_map(mla_step, mesh=mesh, in_specs=in_specs, out_specs=row_spec, check_vma=False)
```

```python
import functools
import math

import jax
import jax.numpy as jnp
from jax import lax
from jax.experimental import pallas as pl
from jax.experimental.pallas import tpu as pltpu
from jax.sharding import PartitionSpec as P

MESH = pl.DeviceIdType.MESH
F32 = jnp.float32
BF16 = jnp.bfloat16
LOWEST = float(jnp.finfo(jnp.float32).min)
DCH = 256
SLOTS = 4
RPC = 2


def iota(shape, dim):
    return lax.broadcasted_iota(jnp.int32, shape, dim)


def dot(a, b):
    return lax.dot_general(a, b, (((1,), (0,)), ((), ())), preferred_element_type=F32)


def dot_nt(a, b):
    return lax.dot_general(a, b, (((1,), (1,)), ((), ())), preferred_element_type=F32)


def merge(blocks, lat):
    rows = []
    for r in range(RPC):
        base = RPC * lat
        ms = [b[:, base + r:base + r + 1] for b in blocks]
        ls = [b[:, base + RPC + r:base + RPC + r + 1] for b in blocks]
        m = functools.reduce(jnp.maximum, ms)
        ws = [jnp.exp(x - m) for x in ms]
        l = functools.reduce(lambda a, b: a + b, [w * y for w, y in zip(ws, ls)])
        o = functools.reduce(lambda a, b: a + b,
                             [w * b[:, r * lat:(r + 1) * lat] for w, b in zip(ws, blocks)])
        rows.append((o, m, l))
    return rows


def pack_ml(ms, ls, shape):
    lane = iota(shape, 1)
    out = jnp.zeros(shape, F32)
    for r in range(RPC):
        out = jnp.where(lane == r, ms[r], out)
        out = jnp.where(lane == RPC + r, ls[r], out)
    return out


def kernel(n, scale, lens, hid_hbm, c_hbm, k_hbm, wuq_hbm, wqr_hbm, wuk_hbm, wuv_hbm, wo_hbm, out_ref,
           hid, hexp, wbuf, wuk, wuv, wo, cb, kb, acc, q_all, qr_st, qr_all, qrow, o_buf, d2d, mid, fin, ol, ovb,
           y_send, y_pair, y_recv, y_own, out_all,
           hid_sem, w_sem, wuk_sem, wqr_sem, c_sem, k_sem, wuv_sem, wo_sem,
           ag_s, ag_r, rs_s, d2d_r, mid_r, fin_r, yp_s, yp_r, y_s, y_r, g_s, g_r):
    s = lax.axis_index("seq")
    x, c = lax.div(s, 2), lax.rem(s, 2)
    nx = n // 2
    oc = 1 - c
    xr, xl, xo = lax.rem(x + 1, nx), lax.rem(x + nx - 1, nx), lax.rem(x + 2, nx)
    partner, right, left = 2 * x + oc, 2 * xr + c, 2 * xl + c
    rows, dm = hid.shape
    t_len, lat = cb.shape[1], cb.shape[2]
    nheads = 16 * n
    nc = dm // DCH
    nch = rows // RPC

    def remote(src, dst, ssem, rsem, dev):
        return pltpu.make_async_remote_copy(src_ref=src, dst_ref=dst, send_sem=ssem, recv_sem=rsem,
                                            device_id={"seq": dev}, device_id_type=MESH)

    def w_copy(g):
        return pltpu.make_async_copy(wuq_hbm.at[pl.ds(g * DCH, DCH)], wbuf.at[lax.rem(g, SLOTS)],
                                     w_sem.at[lax.rem(g, SLOTS)])

    def wuk_copy(half):
        return pltpu.make_async_copy(wuk_hbm.at[half], wuk.at[half], wuk_sem.at[half])

    def wqr_copy(j):
        return pltpu.make_async_copy(wqr_hbm.at[pl.ds(j * 128, 128)], wo.at[pl.ds(j * 128, 128)], wqr_sem.at[j])

    def c_copy(b):
        return pltpu.make_async_copy(c_hbm.at[b], cb.at[b], c_sem.at[b])

    def k_copy(b):
        return pltpu.make_async_copy(k_hbm.at[b], kb.at[b], k_sem.at[b])

    def wo_copy(j):
        return pltpu.make_async_copy(wo_hbm.at[pl.ds(j * 256, 256)], wo.at[pl.ds(j * 256, 256)], wo_sem.at[j])

    hid_copy = pltpu.make_async_copy(hid_hbm, hid, hid_sem)
    hid_copy.start()
    for g in range(SLOTS):
        w_copy(jnp.int32(g)).start()

    barrier = pltpu.get_barrier_semaphore()
    for d in range(1, n):
        pl.semaphore_signal(barrier, inc=1, device_id={"seq": lax.rem(s + d, n)}, device_id_type=MESH)

    hid_copy.wait()
    rep = jnp.where(iota((128, 1024), 0) == lax.div(iota((128, 1024), 1), 8), 1.0, 0.0).astype(BF16)
    ndt = dm // 128
    for g0 in range(0, ndt, 8):
        grp = list(range(g0, min(g0 + 8, ndt)))
        st = jnp.concatenate([hid[:, t * 128:(t + 1) * 128] for t in grp], axis=0)
        ex = dot(st, rep).astype(BF16)
        for i, t in enumerate(grp):
            hexp[:, t * 1024:(t + 1) * 1024] = ex[i * 16:(i + 1) * 16]

    head_mask = jnp.where(lax.div(iota((128, 128), 0), 16) == lax.rem(iota((128, 128), 1), 8), 1.0, 0.0).astype(BF16)
    ri, ci = iota((128, 128), 0), iota((128, 128), 1)
    to_bh = jnp.where(ci == lax.rem(ri, 8) * 16 + lax.div(ri, 8), 1.0, 0.0).astype(BF16)
    to_hb = jnp.where(ci == lax.rem(ri, 16) * 8 + lax.div(ri, 16), 1.0, 0.0).astype(BF16)
    row_h = lax.rem(iota((128, 1), 0), 8)

    opp = 2 * xo + c

    def ag_buf(t, owner):
        return qr_all.at[owner] if t == 4 else q_all.at[owner, t // 2, pl.ds(t % 2 * 64, 64)]

    def ag(t, i, owner, dev):
        return remote(ag_buf(t, owner), ag_buf(t, owner), ag_s.at[t, i], ag_r.at[t, owner], dev)

    def ag_own(half):
        t0, t1 = 2 * half, 2 * half + 1
        for t, i, dev in ((t0, 0, right), (t1, 1, left), (t1, 0, right), (t0, 1, left), (t0, 2, partner),
                          (t1, 2, partner)):
            ag(t, i, s, dev).start()

    def ag_fwd1(half):
        t0, t1 = 2 * half, 2 * half + 1
        ag(t0, 0, left, right).wait_recv()
        ag(t0, 5, left, right).start()
        ag(t0, 3, left, partner).start()
        ag(t1, 1, right, left).wait_recv()
        ag(t1, 5, right, left).start()
        ag(t1, 4, right, partner).start()

    def ag_fwd2(half):
        t0, t1 = 2 * half, 2 * half + 1
        ag(t1, 0, left, right).wait_recv()
        ag(t1, 3, left, partner).start()
        ag(t0, 1, right, left).wait_recv()
        ag(t0, 4, right, partner).start()

    def ag_fwd3(half):
        for t in (2 * half, 2 * half + 1):
            ag(t, 5, opp, right).wait_recv()
            ag(t, 6, opp, partner).start()

    def ag_partner(t):
        for xx in (x, xl, xr, xo):
            ag(t, 2, 2 * xx + oc, partner).wait_recv()

    def ag_done(t):
        for i in range(7):
            ag(t, i, s, partner).wait_send()

    kk = DCH * 8
    acc[...] = jnp.zeros_like(acc)

    @pl.loop(0, nc)
    def _(g):
        slot = lax.rem(g, SLOTS)
        w_copy(g).wait()
        w0 = wbuf[slot, :, 0].reshape(kk, 128)
        w1 = wbuf[slot, :, 1].reshape(kk, 128)
        part = acc[...]
        for q0 in range(0, kk, 1024):
            hx = hexp[:, pl.ds(pl.multiple_of(g * kk + q0, 1024), 1024)]
            lhs = jnp.concatenate([hx] * 8, axis=0) * jnp.concatenate([head_mask] * 8, axis=1)
            part += dot(lhs, jnp.concatenate([w0[q0:q0 + 1024], w1[q0:q0 + 1024]], axis=1))
        acc[...] = part

        @pl.when(g + SLOTS < nc)
        def _():
            w_copy(g + SLOTS).start()

        @pl.when(g >= nc - SLOTS)
        def _():
            for e in range(8 // SLOTS):
                wqr_copy((g - (nc - SLOTS)) * (8 // SLOTS) + e).start()

        @pl.when(g == nc - 2 * SLOTS)
        def _():
            wuk_copy(0).start()
            wuk_copy(1).start()

    for half in range(2):
        qn = dot(to_bh, acc[:, half * 128:(half + 1) * 128].astype(BF16)).astype(BF16)
        wuk_copy(half).wait()
        ql = jnp.zeros((128, lat), F32)
        for h in range(8):
            ql += dot(jnp.where(row_h == h, qn, jnp.zeros_like(qn)), wuk[half, h * 128:(h + 1) * 128, :])
        q_all[s, half] = ql.astype(BF16)
        if half == 0:
            pl.semaphore_wait(barrier, n - 1)
        ag_own(half)

    @pl.loop(0, 8)
    def _(j):
        wqr_copy(j).wait()
        qr = dot_nt(hid[...], wo[pl.ds(pl.multiple_of(j * 128, 128), 128), :])
        qr_st[pl.ds(pl.multiple_of(j * 16, 16), 16), :] = qr.astype(BF16)
        for r in range(2):
            b = 2 * j + r
            c_copy(b).start()
            k_copy(b).start()

        @pl.when(j == 6)
        def _():
            ag_fwd1(0)

    qr_all[s] = dot(to_bh, qr_st[...]).astype(BF16)
    for i, dev in ((0, right), (1, left), (5, opp), (2, partner)):
        ag(4, i, s, dev).start()
    pltpu.make_async_copy(wuv_hbm, wuv, wuv_sem).start()
    ag_fwd1(1)
    ag_fwd2(0)
    ag_fwd2(1)
    for i, owner in ((3, left), (4, right), (6, opp)):
        ag(4, 0, owner, right).wait_recv()
        ag(4, i, owner, partner).start()
    ag_fwd3(0)
    ag_fwd3(1)
    for t in range(5):
        ag_partner(t)

    dup = jnp.where(lax.div(iota((128, 64), 0), 2) == iota((128, 64), 1), 1.0, 0.0).astype(BF16)
    rope_mask = jnp.where(lax.rem(iota((128, 128), 0), 2) == lax.div(iota((128, 128), 1), 64), 1.0, 0.0)
    pos = s * t_len + iota((1, t_len), 1)
    width = RPC * lat + 128

    def attend(k):
        k16 = pl.ds(pl.multiple_of(k * 16, 16), 16)
        for p in range(n):
            qa = q_all[p, 0, k16, :].astype(F32)
            qb = q_all[p, 1, k16, :].astype(F32)
            for r in range(RPC):
                qrow[r, p * 16:(p + 1) * 16, :] = jnp.concatenate(
                    [qa[r * 8:(r + 1) * 8], qb[r * 8:(r + 1) * 8]], axis=0).astype(BF16)
        mls = []
        for r in range(RPC):
            b = k * RPC + r
            c_copy(b).wait()
            k_copy(b).wait()
            pairs = jnp.concatenate(
                [qr_all[p, k16, :].astype(F32)[r * 8:(r + 1) * 8] for p in range(n)], axis=0).astype(BF16)
            qr = (dot(dup, pairs) * rope_mask).astype(BF16)
            keys = kb[b]
            sc = dot_nt(qrow[r], cb[b]) + dot(qr, jnp.concatenate([keys, keys], axis=0))
            sc = jnp.where(pos < lens[b], sc * scale, -jnp.inf)
            m = jnp.maximum(jnp.max(sc, axis=1, keepdims=True), LOWEST)
            pw = jnp.exp(sc - m)
            l = jnp.sum(pw, axis=1, keepdims=True)
            o = dot(pw.astype(BF16), cb[b])
            for p in range(n):
                for ab in range(2):
                    h0 = p * 16 + ab * 8
                    o_buf[k, p % 2, p // 2, ab, :, r * lat:(r + 1) * lat] = o[h0:h0 + 8]
            mls.append((m, l))
        ml = pack_ml([a for a, _ in mls], [a for _, a in mls], (nheads, 128))
        for p in range(n):
            for ab in range(2):
                h0 = p * 16 + ab * 8
                o_buf[k, p % 2, p // 2, ab, :, RPC * lat:] = ml[h0:h0 + 8]

    def d2d_copy(k):
        return remote(o_buf.at[k, oc], d2d.at[k], rs_s.at[k, 0], d2d_r.at[k], partner)

    def hop_copies(k):
        return [
            remote(o_buf.at[k, c, xo, 1], mid.at[k, 0], rs_s.at[k, 1], mid_r.at[k, 0], right),
            remote(o_buf.at[k, c, xo, 0], mid.at[k, 1], rs_s.at[k, 2], mid_r.at[k, 1], left),
            remote(o_buf.at[k, c, xr, 0], fin.at[k, 0], rs_s.at[k, 3], fin_r.at[k, 0], right),
            remote(o_buf.at[k, c, xl, 1], fin.at[k, 1], rs_s.at[k, 4], fin_r.at[k, 1], left),
        ]

    def mid_copies(k):
        return [
            remote(o_buf.at[k, c, xr, 1], fin.at[k, 2], rs_s.at[k, 5], fin_r.at[k, 2], right),
            remote(o_buf.at[k, c, xl, 0], fin.at[k, 3], rs_s.at[k, 6], fin_r.at[k, 3], left),
        ]

    def store_merged(k, xx, ab, other):
        ref = o_buf.at[k, c, xx, ab]
        res = merge([ref[...], other], lat)
        for r in range(RPC):
            ref[:, r * lat:(r + 1) * lat] = res[r][0]
        ref[:, RPC * lat:] = pack_ml([a[1] for a in res], [a[2] for a in res], (8, 128))

    def pair_stage(k):
        d2d_copy(k).wait_recv()
        for xx in range(nx):
            for ab in range(2):
                store_merged(k, xx, ab, d2d[k, xx, ab])
        for cp in hop_copies(k):
            cp.start()

    def mid_stage(k):
        hops, mids = hop_copies(k), mid_copies(k)
        hops[0].wait_recv()
        store_merged(k, xr, 1, mid[k, 0])
        mids[0].start()
        hops[1].wait_recv()
        store_merged(k, xl, 0, mid[k, 1])
        mids[1].start()

    def final_stage(k):
        hops, mids = hop_copies(k), mid_copies(k)
        hops[2].wait_recv()
        hops[3].wait_recv()
        mids[0].wait_recv()
        mids[1].wait_recv()
        for ab, (f0, f1) in enumerate(((0, 3), (1, 2))):
            res = merge([o_buf[k, c, x, ab], fin[k, f0], fin[k, f1]], lat)
            ol[ab, pl.ds(pl.multiple_of(k * 16, 16), 16), :] = jnp.concatenate(
                [o / l for o, _, l in res], axis=0).astype(BF16)

    @pl.loop(0, nch + 5)
    def _(k):
        @pl.when(k < nch)
        def _():
            attend(k)
            d2d_copy(k).start()
            wo_copy(k).start()

        @pl.when((k >= 1) & (k < nch + 1))
        def _():
            pair_stage(k - 1)

        @pl.when((k >= 3) & (k < nch + 3))
        def _():
            mid_stage(k - 3)

        @pl.when(k >= 5)
        def _():
            final_stage(k - 5)

    pltpu.make_async_copy(wuv_hbm, wuv, wuv_sem).wait()
    for ab in range(2):
        ov = jnp.zeros((128, 128), F32)
        src = ol[ab]
        for h in range(8):
            ov += dot(jnp.where(row_h == h, src, jnp.zeros_like(src)), wuv[ab, h * lat:(h + 1) * lat, :])
        ov = dot(to_hb, ov.astype(BF16)).astype(BF16)
        for h in range(8):
            ovb[:, (ab * 8 + h) * 128:(ab * 8 + h + 1) * 128] = ov[h * 16:(h + 1) * 16]
    for j in range(8):
        wo_copy(j).wait()

    yw = dm // n

    def y_block(p):
        return dot(ovb[...], wo[:, pl.ds(pl.multiple_of(p * yw, yw), yw)])

    def yp_copy(xx):
        return remote(y_send.at[2 * xx + oc], y_pair.at[xx], yp_s.at[xx], yp_r.at[xx], partner)

    def y_copy(xx):
        return remote(y_send.at[2 * xx + c], y_recv.at[x], y_s.at[xx], y_r.at[x], 2 * xx + c)

    @pl.loop(0, nx)
    def _(i):
        xx = lax.rem(x + nx - 1 - i, nx)
        y_send[2 * xx + oc] = y_block(2 * xx + oc)
        yp_copy(xx).start()

    @pl.loop(0, nx)
    def _(i):
        xx = lax.rem(x + nx - 1 - i, nx)
        blk = y_block(2 * xx + c)
        yp_copy(xx).wait_recv()
        y_send[2 * xx + c] = blk + y_pair[xx]

        @pl.when(i < nx - 1)
        def _():
            y_copy(xx).start()

    y = y_send[s]
    for xx in (xr, xl, xo):
        remote(y_send.at[s], y_recv.at[xx], y_s.at[xx], y_r.at[xx], right).wait_recv()
        y += y_recv[xx]
    y += hid[:, pl.ds(pl.multiple_of(s * yw, yw), yw)].astype(F32)
    y_own[...] = y.astype(BF16)

    def g_copy(d):
        dev = lax.rem(s + d, n)
        return remote(y_own, out_all.at[s], g_s.at[dev], g_r.at[s], dev)

    for d in range(1, n):
        g_copy(d).start()
    out_ref[:, pl.ds(pl.multiple_of(s * yw, yw), yw)] = y_own[...]
    for d in range(1, n):
        src = lax.rem(s + d, n)
        remote(y_own, out_all.at[src], g_s.at[src], g_r.at[src], src).wait_recv()
        out_ref[:, pl.ds(pl.multiple_of(src * yw, yw), yw)] = out_all[src]

    for t in range(5):
        ag_done(t)

    @pl.loop(0, nch)
    def _(k):
        d2d_copy(k).wait_send()
        for cp in hop_copies(k) + mid_copies(k):
            cp.wait_send()

    for xx in range(nx):
        yp_copy(xx).wait_send()
    for xx in (xr, xl, xo):
        y_copy(xx).wait_send()
    for d in range(1, n):
        g_copy(d).wait_send()


def solution(mesh):
    n = mesh.shape['seq']
    row_spec = P('batch', None)
    cache_spec = P('batch', 'seq', None)
    in_specs = (row_spec, P('batch'), cache_spec, cache_spec, P(None, 'seq', None), P(None, 'seq', None),
                P('seq', None, None), P('seq', None, None), P('seq', None, None))

    def mla_step(hidden, lengths, c_kv, k_rope, w_uq, w_qr, w_uk, w_uv, w_o):
        rows, dm = hidden.shape
        t_len, lat = c_kv.shape[1:]
        rope = k_rope.shape[2]
        nh, nope = w_uq.shape[1:]
        vdim = w_uv.shape[2]
        scale = 1.0 / math.sqrt(nope + rope)
        nch, yw, width = rows // RPC, dm // n, RPC * lat + 128
        any_spec = pl.BlockSpec(memory_space=pl.ANY)
        vmem = pl.BlockSpec(memory_space=pltpu.VMEM)
        dma, V = pltpu.SemaphoreType.DMA, pltpu.VMEM
        return pl.pallas_call(
            functools.partial(kernel, n, scale),
            out_shape=jax.ShapeDtypeStruct((rows, dm), BF16),
            in_specs=[pl.BlockSpec(memory_space=pltpu.SMEM)] + [any_spec] * 8,
            out_specs=vmem,
            scratch_shapes=[
                V((rows, dm), BF16), V((rows, dm * 8), BF16), V((SLOTS, DCH, 2, 8, nope), BF16), V((2, 8 * nope, lat), BF16),
                V((2, 8 * lat, vdim), BF16), V((nh * vdim, dm), BF16), V((rows, t_len, lat), BF16),
                V((rows, rope, t_len), BF16), V((128, 2 * nope), F32), V((n, 2, 128, lat), BF16),
                V((128, 128), BF16), V((n, 128, 128), BF16), V((RPC, nh * n, lat), BF16),
                V((nch, 2, n // 2, 2, 8, width), F32), V((nch, n // 2, 2, 8, width), F32),
                V((nch, 2, 8, width), F32), V((nch, 4, 8, width), F32), V((2, 128, lat), BF16),
                V((rows, nh * vdim), BF16), V((n, rows, yw), F32), V((n // 2, rows, yw), F32), V((n // 2, rows, yw), F32),
                V((rows, yw), BF16), V((n, rows, yw), BF16),
                dma(()), dma((SLOTS,)), dma((2,)), dma((8,)), dma((rows,)), dma((rows,)), dma(()), dma((8,)),
                dma((5, 7)), dma((5, n)), dma((nch, 7)), dma((nch,)), dma((nch, 2)), dma((nch, 4)),
                dma((n // 2,)), dma((n // 2,)), dma((n // 2,)), dma((n // 2,)), dma((n,)), dma((n,)),
            ],
            compiler_params=pltpu.CompilerParams(collective_id=0, has_side_effects=True,
                                                 vmem_limit_bytes=67043328),
        )(lengths, hidden, c_kv, jnp.swapaxes(k_rope, 1, 2), w_uq.reshape(dm, 2, nh // 2, nope),
          jnp.transpose(w_qr, (1, 2, 0)).reshape(nh * rope, dm), w_uk.reshape(2, nh // 2 * nope, lat),
          w_uv.reshape(2, nh // 2 * lat, vdim), w_o.reshape(nh * vdim, dm))

    return jax.shard_map(mla_step, mesh=mesh, in_specs=in_specs, out_specs=row_spec, check_vma=False)
```

```python
import functools
import math

import jax
import jax.numpy as jnp
from jax import lax
from jax.experimental import pallas as pl
from jax.experimental.pallas import tpu as pltpu
from jax.sharding import PartitionSpec as P

MESH = pl.DeviceIdType.MESH
F32 = jnp.float32
BF16 = jnp.bfloat16
LOWEST = float(jnp.finfo(jnp.float32).min)
DCH = 512
SLOTS = 4
RPC = 2


def iota(shape, dim):
    return lax.broadcasted_iota(jnp.int32, shape, dim)


def dot(a, b):
    return lax.dot_general(a, b, (((1,), (0,)), ((), ())), preferred_element_type=F32)


def dot_nt(a, b):
    return lax.dot_general(a, b, (((1,), (1,)), ((), ())), preferred_element_type=F32)


def merge(blocks, lat):
    rows = []
    for r in range(RPC):
        base = RPC * lat
        ms = [b[:, base + r:base + r + 1] for b in blocks]
        ls = [b[:, base + RPC + r:base + RPC + r + 1] for b in blocks]
        m = functools.reduce(jnp.maximum, ms)
        ws = [jnp.exp(x - m) for x in ms]
        l = functools.reduce(lambda a, b: a + b, [w * y for w, y in zip(ws, ls)])
        o = functools.reduce(lambda a, b: a + b,
                             [w * b[:, r * lat:(r + 1) * lat] for w, b in zip(ws, blocks)])
        rows.append((o, m, l))
    return rows


def pack_ml(ms, ls, shape):
    lane = iota(shape, 1)
    out = jnp.zeros(shape, F32)
    for r in range(RPC):
        out = jnp.where(lane == r, ms[r], out)
        out = jnp.where(lane == RPC + r, ls[r], out)
    return out


def kernel(n, scale, lens, hid_hbm, c_hbm, k_hbm, wuq_hbm, wqr_hbm, wuk_hbm, wuv_hbm, wo_hbm, out_ref,
           hid, hexp, wbuf, wuk, wuv, wo, cb, kb, acc, q_all, qr_st, qr_all, qrow, o_buf, d2d, mid, fin, ol, ovb,
           y_send, y_pair, y_recv, y_own, out_all,
           hid_sem, w_sem, wuk_sem, wqr_sem, c_sem, k_sem, wuv_sem, wo_sem,
           ag_s, ag_r, rs_s, d2d_r, mid_r, fin_r, yp_s, yp_r, y_s, y_r, g_s, g_r):
    s = lax.axis_index("seq")
    x, c = lax.div(s, 2), lax.rem(s, 2)
    nx = n // 2
    oc = 1 - c
    xr, xl, xo = lax.rem(x + 1, nx), lax.rem(x + nx - 1, nx), lax.rem(x + 2, nx)
    partner, right, left = 2 * x + oc, 2 * xr + c, 2 * xl + c
    rows, dm = hid.shape
    t_len, lat = cb.shape[1], cb.shape[2]
    nheads = 16 * n
    nc = dm // DCH
    nch = rows // RPC

    def remote(src, dst, ssem, rsem, dev):
        return pltpu.make_async_remote_copy(src_ref=src, dst_ref=dst, send_sem=ssem, recv_sem=rsem,
                                            device_id={"seq": dev}, device_id_type=MESH)

    def w_copy(g):
        half, i = lax.div(g, nc), lax.rem(g, nc)
        return pltpu.make_async_copy(wuq_hbm.at[pl.ds(i * DCH, DCH), half], wbuf.at[lax.rem(g, SLOTS)],
                                     w_sem.at[lax.rem(g, SLOTS)])

    def wuk_copy(half):
        return pltpu.make_async_copy(wuk_hbm.at[half], wuk.at[half], wuk_sem.at[half])

    def wqr_copy(j):
        return pltpu.make_async_copy(wqr_hbm.at[pl.ds(j * 128, 128)], wo.at[pl.ds(j * 128, 128)], wqr_sem.at[j])

    def c_copy(b):
        return pltpu.make_async_copy(c_hbm.at[b], cb.at[b], c_sem.at[b])

    def k_copy(b):
        return pltpu.make_async_copy(k_hbm.at[b], kb.at[b], k_sem.at[b])

    def wo_copy(j):
        return pltpu.make_async_copy(wo_hbm.at[pl.ds(j * 256, 256)], wo.at[pl.ds(j * 256, 256)], wo_sem.at[j])

    hid_copy = pltpu.make_async_copy(hid_hbm, hid, hid_sem)
    hid_copy.start()
    for g in range(SLOTS):
        w_copy(jnp.int32(g)).start()
    wuk_copy(0).start()

    barrier = pltpu.get_barrier_semaphore()
    for d in range(1, n):
        pl.semaphore_signal(barrier, inc=1, device_id={"seq": lax.rem(s + d, n)}, device_id_type=MESH)

    hid_copy.wait()
    rep = jnp.where(iota((128, 1024), 0) == lax.div(iota((128, 1024), 1), 8), 1.0, 0.0).astype(BF16)
    ndt = dm // 128
    for g0 in range(0, ndt, 8):
        grp = list(range(g0, min(g0 + 8, ndt)))
        st = jnp.concatenate([hid[:, t * 128:(t + 1) * 128] for t in grp], axis=0)
        ex = dot(st, rep).astype(BF16)
        for i, t in enumerate(grp):
            hexp[:, t * 1024:(t + 1) * 1024] = ex[i * 16:(i + 1) * 16]

    head_mask = jnp.where(lax.div(iota((128, 128), 0), 16) == lax.rem(iota((128, 128), 1), 8), 1.0, 0.0).astype(BF16)
    ri, ci = iota((128, 128), 0), iota((128, 128), 1)
    to_bh = jnp.where(ci == lax.rem(ri, 8) * 16 + lax.div(ri, 8), 1.0, 0.0).astype(BF16)
    to_hb = jnp.where(ci == lax.rem(ri, 16) * 8 + lax.div(ri, 16), 1.0, 0.0).astype(BF16)
    row_h = lax.rem(iota((128, 1), 0), 8)

    opp = 2 * xo + c

    def ag_buf(t, owner):
        return qr_all.at[owner] if t == 4 else q_all.at[owner, t // 2, pl.ds(t % 2 * 64, 64)]

    def ag(t, i, owner, dev):
        return remote(ag_buf(t, owner), ag_buf(t, owner), ag_s.at[t, i], ag_r.at[t, owner], dev)

    def ag_own(half):
        t0, t1 = 2 * half, 2 * half + 1
        for t, i, dev in ((t0, 0, right), (t1, 1, left), (t1, 0, right), (t0, 1, left), (t0, 2, partner),
                          (t1, 2, partner)):
            ag(t, i, s, dev).start()

    def ag_fwd1(half):
        t0, t1 = 2 * half, 2 * half + 1
        ag(t0, 0, left, right).wait_recv()
        ag(t0, 5, left, right).start()
        ag(t0, 3, left, partner).start()
        ag(t1, 1, right, left).wait_recv()
        ag(t1, 5, right, left).start()
        ag(t1, 4, right, partner).start()

    def ag_fwd2(half):
        t0, t1 = 2 * half, 2 * half + 1
        ag(t1, 0, left, right).wait_recv()
        ag(t1, 3, left, partner).start()
        ag(t0, 1, right, left).wait_recv()
        ag(t0, 4, right, partner).start()

    def ag_fwd3(half):
        for t in (2 * half, 2 * half + 1):
            ag(t, 5, opp, right).wait_recv()
            ag(t, 6, opp, partner).start()

    def ag_partner(t):
        for xx in (x, xl, xr, xo):
            ag(t, 2, 2 * xx + oc, partner).wait_recv()

    def ag_done(t):
        for i in range(7):
            ag(t, i, s, partner).wait_send()

    kk = DCH * 8
    def half_step(half):
        acc[...] = jnp.zeros_like(acc)

        @pl.loop(0, nc)
        def _(i):
            g = half * nc + i
            slot = lax.rem(g, SLOTS)
            w_copy(g).wait()
            wv = wbuf[slot].reshape(kk, 128)
            part = acc[...]
            for q0 in range(0, kk, 512):
                hx = hexp[:, pl.ds(pl.multiple_of(i * kk + q0, 512), 512)]
                lhs = jnp.concatenate([hx] * 8, axis=0) * jnp.concatenate([head_mask] * 4, axis=1)
                part += dot(lhs, wv[q0:q0 + 512])
            acc[...] = part

            @pl.when(g + SLOTS < 2 * nc)
            def _():
                w_copy(g + SLOTS).start()

            @pl.when(g >= 2 * nc - SLOTS)
            def _():
                for e in range(8 // SLOTS):
                    wqr_copy((g - (2 * nc - SLOTS)) * (8 // SLOTS) + e).start()

            if half == 0:
                @pl.when(i == 1)
                def _():
                    wuk_copy(1).start()
            else:
                @pl.when(i == nc - 1)
                def _():
                    ag_fwd1(0)

        qn = dot(to_bh, acc[...].astype(BF16)).astype(BF16)
        wuk_copy(half).wait()
        ql = jnp.zeros((128, lat), F32)
        for h in range(8):
            ql += dot(jnp.where(row_h == h, qn, jnp.zeros_like(qn)), wuk[half, h * 128:(h + 1) * 128, :])
        q_all[s, half] = ql.astype(BF16)
        if half == 0:
            pl.semaphore_wait(barrier, n - 1)
        ag_own(half)

    half_step(0)
    half_step(1)

    @pl.loop(0, 4)
    def _(j):
        wqr_copy(2 * j).wait()
        wqr_copy(2 * j + 1).wait()
        qr = dot_nt(hid[...], wo[pl.ds(pl.multiple_of(j * 256, 256), 256), :]).astype(BF16)
        qr_st[pl.ds(pl.multiple_of(j * 32, 32), 32), :] = jnp.concatenate([qr[:, :128], qr[:, 128:]], axis=0)
        for r in range(4):
            b = 4 * j + r
            c_copy(b).start()
            k_copy(b).start()

        @pl.when(j == 1)
        def _():
            ag_fwd2(0)

        @pl.when(j == 3)
        def _():
            ag_fwd3(0)

    qr_all[s] = dot(to_bh, qr_st[...]).astype(BF16)
    for i, dev in ((0, right), (1, left), (5, opp), (2, partner)):
        ag(4, i, s, dev).start()
    pltpu.make_async_copy(wuv_hbm, wuv, wuv_sem).start()
    ag_fwd1(1)
    ag_fwd2(1)
    for i, owner in ((3, left), (4, right), (6, opp)):
        ag(4, 0, owner, right).wait_recv()
        ag(4, i, owner, partner).start()
    ag_fwd3(1)
    for t in range(5):
        ag_partner(t)

    dup = jnp.where(lax.div(iota((128, 64), 0), 2) == iota((128, 64), 1), 1.0, 0.0).astype(BF16)
    rope_mask = jnp.where(lax.rem(iota((128, 128), 0), 2) == lax.div(iota((128, 128), 1), 64), 1.0, 0.0)
    pos = s * t_len + iota((1, t_len), 1)
    width = RPC * lat + 128

    def attend(k):
        k16 = pl.ds(pl.multiple_of(k * 16, 16), 16)
        for p in range(n):
            qa = q_all[p, 0, k16, :].astype(F32)
            qb = q_all[p, 1, k16, :].astype(F32)
            for r in range(RPC):
                qrow[r, p * 16:(p + 1) * 16, :] = jnp.concatenate(
                    [qa[r * 8:(r + 1) * 8], qb[r * 8:(r + 1) * 8]], axis=0).astype(BF16)
        mls = []
        for r in range(RPC):
            b = k * RPC + r
            c_copy(b).wait()
            k_copy(b).wait()
            pairs = jnp.concatenate(
                [qr_all[p, k16, :].astype(F32)[r * 8:(r + 1) * 8] for p in range(n)], axis=0).astype(BF16)
            qr = (dot(dup, pairs) * rope_mask).astype(BF16)
            keys = kb[b]
            sc = dot_nt(qrow[r], cb[b]) + dot(qr, jnp.concatenate([keys, keys], axis=0))
            sc = jnp.where(pos < lens[b], sc * scale, -jnp.inf)
            m = jnp.maximum(jnp.max(sc, axis=1, keepdims=True), LOWEST)
            pw = jnp.exp(sc - m)
            l = jnp.sum(pw, axis=1, keepdims=True)
            o = dot(pw.astype(BF16), cb[b])
            for p in range(n):
                for ab in range(2):
                    h0 = p * 16 + ab * 8
                    o_buf[k, p % 2, p // 2, ab, :, r * lat:(r + 1) * lat] = o[h0:h0 + 8]
            mls.append((m, l))
        ml = pack_ml([a for a, _ in mls], [a for _, a in mls], (nheads, 128))
        for p in range(n):
            for ab in range(2):
                h0 = p * 16 + ab * 8
                o_buf[k, p % 2, p // 2, ab, :, RPC * lat:] = ml[h0:h0 + 8]

    def d2d_copy(k):
        return remote(o_buf.at[k, oc], d2d.at[k], rs_s.at[k, 0], d2d_r.at[k], partner)

    def hop_copies(k):
        return [
            remote(o_buf.at[k, c, xo, 1], mid.at[k, 0], rs_s.at[k, 1], mid_r.at[k, 0], right),
            remote(o_buf.at[k, c, xo, 0], mid.at[k, 1], rs_s.at[k, 2], mid_r.at[k, 1], left),
            remote(o_buf.at[k, c, xr, 0], fin.at[k, 0], rs_s.at[k, 3], fin_r.at[k, 0], right),
            remote(o_buf.at[k, c, xl, 1], fin.at[k, 1], rs_s.at[k, 4], fin_r.at[k, 1], left),
        ]

    def mid_copies(k):
        return [
            remote(o_buf.at[k, c, xr, 1], fin.at[k, 2], rs_s.at[k, 5], fin_r.at[k, 2], right),
            remote(o_buf.at[k, c, xl, 0], fin.at[k, 3], rs_s.at[k, 6], fin_r.at[k, 3], left),
        ]

    def store_merged(k, xx, ab, other):
        ref = o_buf.at[k, c, xx, ab]
        res = merge([ref[...], other], lat)
        for r in range(RPC):
            ref[:, r * lat:(r + 1) * lat] = res[r][0]
        ref[:, RPC * lat:] = pack_ml([a[1] for a in res], [a[2] for a in res], (8, 128))

    def pair_stage(k):
        d2d_copy(k).wait_recv()
        for xx in range(nx):
            for ab in range(2):
                store_merged(k, xx, ab, d2d[k, xx, ab])
        for cp in hop_copies(k):
            cp.start()

    def mid_stage(k):
        hops, mids = hop_copies(k), mid_copies(k)
        hops[0].wait_recv()
        store_merged(k, xr, 1, mid[k, 0])
        mids[0].start()
        hops[1].wait_recv()
        store_merged(k, xl, 0, mid[k, 1])
        mids[1].start()

    def final_stage(k):
        hops, mids = hop_copies(k), mid_copies(k)
        hops[2].wait_recv()
        hops[3].wait_recv()
        mids[0].wait_recv()
        mids[1].wait_recv()
        for ab, (f0, f1) in enumerate(((0, 3), (1, 2))):
            res = merge([o_buf[k, c, x, ab], fin[k, f0], fin[k, f1]], lat)
            ol[ab, pl.ds(pl.multiple_of(k * 16, 16), 16), :] = jnp.concatenate(
                [o / l for o, _, l in res], axis=0).astype(BF16)

    @pl.loop(0, nch + 5)
    def _(k):
        @pl.when(k < nch)
        def _():
            attend(k)
            d2d_copy(k).start()
            wo_copy(k).start()

        @pl.when((k >= 1) & (k < nch + 1))
        def _():
            pair_stage(k - 1)

        @pl.when((k >= 3) & (k < nch + 3))
        def _():
            mid_stage(k - 3)

        @pl.when(k >= 5)
        def _():
            final_stage(k - 5)

    pltpu.make_async_copy(wuv_hbm, wuv, wuv_sem).wait()
    for ab in range(2):
        ov = jnp.zeros((128, 128), F32)
        src = ol[ab]
        for h in range(8):
            ov += dot(jnp.where(row_h == h, src, jnp.zeros_like(src)), wuv[ab, h * lat:(h + 1) * lat, :])
        ov = dot(to_hb, ov.astype(BF16)).astype(BF16)
        for h in range(8):
            ovb[:, (ab * 8 + h) * 128:(ab * 8 + h + 1) * 128] = ov[h * 16:(h + 1) * 16]
    for j in range(8):
        wo_copy(j).wait()

    yw = dm // n

    def y_block(p):
        return dot(ovb[...], wo[:, pl.ds(pl.multiple_of(p * yw, yw), yw)])

    def chip_at(i):
        q = lax.div(i, 2)
        return lax.rem(x + (1 - q) * (2 + i) + q * (3 - i), nx)

    def yp_copy(xx):
        return remote(y_send.at[2 * xx + oc], y_pair.at[xx], yp_s.at[xx], yp_r.at[xx], partner)

    def y_copy(xx):
        return remote(y_send.at[2 * xx + c], y_recv.at[x], y_s.at[xx], y_r.at[x], 2 * xx + c)

    @pl.loop(0, nx)
    def _(i):
        xx = chip_at(i)
        y_send[2 * xx + oc] = y_block(2 * xx + oc)
        yp_copy(xx).start()

    @pl.loop(0, nx)
    def _(i):
        xx = chip_at(i)
        blk = y_block(2 * xx + c)
        yp_copy(xx).wait_recv()
        y_send[2 * xx + c] = blk + y_pair[xx]

        @pl.when(i < nx - 1)
        def _():
            y_copy(xx).start()

    y = y_send[s]
    for xx in (xr, xl, xo):
        remote(y_send.at[s], y_recv.at[xx], y_s.at[xx], y_r.at[xx], right).wait_recv()
        y += y_recv[xx]
    y += hid[:, pl.ds(pl.multiple_of(s * yw, yw), yw)].astype(F32)
    y_own[...] = y.astype(BF16)

    others = (2 * xo + c, 2 * xo + oc, right, left, 2 * xr + oc, 2 * xl + oc, partner)

    def g_copy(dev):
        return remote(y_own, out_all.at[s], g_s.at[dev], g_r.at[s], dev)

    for dev in others:
        g_copy(dev).start()
    out_ref[:, pl.ds(pl.multiple_of(s * yw, yw), yw)] = y_own[...]
    for src in others:
        remote(y_own, out_all.at[src], g_s.at[src], g_r.at[src], src).wait_recv()
        out_ref[:, pl.ds(pl.multiple_of(src * yw, yw), yw)] = out_all[src]

    for t in range(5):
        ag_done(t)

    @pl.loop(0, nch)
    def _(k):
        d2d_copy(k).wait_send()
        for cp in hop_copies(k) + mid_copies(k):
            cp.wait_send()

    for xx in range(nx):
        yp_copy(xx).wait_send()
    for xx in (xr, xl, xo):
        y_copy(xx).wait_send()
    for dev in others:
        g_copy(dev).wait_send()


def solution(mesh):
    n = mesh.shape['seq']
    row_spec = P('batch', None)
    cache_spec = P('batch', 'seq', None)
    in_specs = (row_spec, P('batch'), cache_spec, cache_spec, P(None, 'seq', None), P(None, 'seq', None),
                P('seq', None, None), P('seq', None, None), P('seq', None, None))

    def mla_step(hidden, lengths, c_kv, k_rope, w_uq, w_qr, w_uk, w_uv, w_o):
        rows, dm = hidden.shape
        t_len, lat = c_kv.shape[1:]
        rope = k_rope.shape[2]
        nh, nope = w_uq.shape[1:]
        vdim = w_uv.shape[2]
        scale = 1.0 / math.sqrt(nope + rope)
        nch, yw, width = rows // RPC, dm // n, RPC * lat + 128
        any_spec = pl.BlockSpec(memory_space=pl.ANY)
        vmem = pl.BlockSpec(memory_space=pltpu.VMEM)
        dma, V = pltpu.SemaphoreType.DMA, pltpu.VMEM
        return pl.pallas_call(
            functools.partial(kernel, n, scale),
            out_shape=jax.ShapeDtypeStruct((rows, dm), BF16),
            in_specs=[pl.BlockSpec(memory_space=pltpu.SMEM)] + [any_spec] * 8,
            out_specs=vmem,
            scratch_shapes=[
                V((rows, dm), BF16), V((rows, dm * 8), BF16), V((SLOTS, DCH, 8, nope), BF16), V((2, 8 * nope, lat), BF16),
                V((2, 8 * lat, vdim), BF16), V((nh * vdim, dm), BF16), V((rows, t_len, lat), BF16),
                V((rows, rope, t_len), BF16), V((128, nope), F32), V((n, 2, 128, lat), BF16),
                V((128, 128), BF16), V((n, 128, 128), BF16), V((RPC, nh * n, lat), BF16),
                V((nch, 2, n // 2, 2, 8, width), F32), V((nch, n // 2, 2, 8, width), F32),
                V((nch, 2, 8, width), F32), V((nch, 4, 8, width), F32), V((2, 128, lat), BF16),
                V((rows, nh * vdim), BF16), V((n, rows, yw), F32), V((n // 2, rows, yw), F32), V((n // 2, rows, yw), F32),
                V((rows, yw), BF16), V((n, rows, yw), BF16),
                dma(()), dma((SLOTS,)), dma((2,)), dma((8,)), dma((rows,)), dma((rows,)), dma(()), dma((8,)),
                dma((5, 7)), dma((5, n)), dma((nch, 7)), dma((nch,)), dma((nch, 2)), dma((nch, 4)),
                dma((n // 2,)), dma((n // 2,)), dma((n // 2,)), dma((n // 2,)), dma((n,)), dma((n,)),
            ],
            compiler_params=pltpu.CompilerParams(collective_id=0, has_side_effects=True,
                                                 vmem_limit_bytes=67043328),
        )(lengths, hidden, c_kv, jnp.swapaxes(k_rope, 1, 2), w_uq.reshape(dm, 2, nh // 2, nope),
          jnp.transpose(w_qr, (1, 2, 0)).reshape(nh * rope, dm), w_uk.reshape(2, nh // 2 * nope, lat),
          w_uv.reshape(2, nh // 2 * lat, vdim), w_o.reshape(nh * vdim, dm))

    return jax.shard_map(mla_step, mesh=mesh, in_specs=in_specs, out_specs=row_spec, check_vma=False)
```
